32 devices in a mesh: band: 2 (over y), strip: 4 (over z), src: 4 (over x, core).
Axes of the slice: x: 2, y: 2, z: 4, core: 2. Of those that a mesh axis runs over, the one named last changes fastest.
Arguments:
- theta: float32 [1024, 512], P(('band', 'strip')), parts along dimension 0, may hold values from -8 to 8
- target: int32 [1024, 512], P(('band', 'strip')), parts along dimension 0, may hold values 0 or 1
- source_shift: int32 [32, 2], P('src'), may hold values from -16 to 16
- source_weight: float32 [32], P('src'), may hold values from 0.14 to 7.1
Outputs:
- theta_final: float32 [1024, 512], P(('band', 'strip')), parts along dimension 0
- resist: float32 [1024, 512], P(('band', 'strip')), parts along dimension 0
The draws below stay inside these ranges and needn't reach their ends.
There are 2 independent parts, one for each index of `band`. The reference program is written for one: setup_inputs(seed, part) draws one part's arguments, and reference() takes and returns one part's arrays. A program takes and returns all parts, laid end to end along the dimension named above; an argument that names none is the same for every part. Nothing has to cross between parts.
All inputs are finite; a program needn't handle non-finite values. No bound on the sum of `target` on one device may be relied on, other than what follows from the above.
Results may differ from the reference program's by a relative error of at most 0.0055.
The reference program's roundings to bfloat16 on the way count: a program that leaves them out, or rounds other values in their place, can miss the bound.
Values may be sent and summed in bfloat16 or wider, within the bound.
No kernel may reach another device: no remote copies, remote signals or barrier semaphores. Data moves between devices by JAX's collectives and lax.ppermute only.
A program may use at most 64 MiB of HBM per device.

```python
import math
import jax
import jax.numpy as jnp
from jax import lax

ROWS = 128
COLS = 512
HALO = 64
FREQ = 128
ITERS = 2
SOURCES = 32
NR = 512
N_STRIP = 4


def draw_source_weight(key, part):
    position = jnp.arange(SOURCES, dtype=jnp.float32) / max(SOURCES - 1, 1)
    jitter = jax.random.uniform(jax.random.fold_in(key, 7), (SOURCES,), jnp.float32, -0.0969, 0.0969)
    exponent = -0.5 + position
    return (10.0 ** (exponent + jitter)).astype(jnp.float32)


def touch_ends(drawn, own_key, least, largest):
    shape = drawn.shape
    place = [jax.random.randint(jax.random.fold_in(own_key, axis), (), 0, shape[axis]) for axis in range(len(shape))]
    drawn = drawn.at[tuple(place)].set(least)
    longest = shape.index(max(shape))
    place[longest] = (place[longest] + 1) % shape[longest]
    return drawn.at[tuple(place)].set(largest)


def shard_levels(rng, shape, shards, low, high):
    gain, own = 1.0, jax.random.fold_in(rng, 6)
    for dim, blocks in shards:
        steps = jnp.exp(jax.random.uniform(jax.random.fold_in(own, dim), (blocks,), jnp.float32, low / len(shards), high / len(shards)))
        gain = gain * jnp.repeat(steps, shape[dim] // blocks).reshape([-1 if axis == dim else 1 for axis in range(len(shape))])
    return gain


def bell_draw(own_key, dims, deviation, limit, shards=(), held_as=jnp.bfloat16):
    values = jax.random.normal(own_key, dims, jnp.float32) * deviation
    if len(shards) > 0:
        values = shard_levels(own_key, dims, shards, -0.22, 0.18) * values
    return jnp.clip(values, min=-limit, max=limit).astype(held_as)


def setup_inputs(seed: int = 0, part: int = 0) -> dict:
    key_of = jax.random.split(jax.random.key(seed), 5)
    part_splits = jax.random.split(jax.random.fold_in(key_of[4], part), 5)
    return {
        "theta": bell_draw(part_splits[0], (NR, COLS), 2.0, 8.0, ((0, 4),), jnp.float32),
        "target": touch_ends((jax.random.randint(part_splits[1], (NR, COLS), 0, 2) < 1).astype(jnp.int32), jax.random.fold_in(part_splits[1], 1), 0, 1),
        "source_shift": touch_ends(jax.random.randint(key_of[2], (SOURCES, 2), -(FREQ // 8), FREQ // 8 + 1), jax.random.fold_in(key_of[2], 1), -(FREQ // 8), (FREQ // 8 + 1) - 1).astype(jnp.int32),
        "source_weight": draw_source_weight(jax.random.fold_in(key_of[4], 71), part),
    }


steepness = 20.0
dose_level = 0.27
step_size = 1.0
epsilon = 1e-06

def phase_pair(freq_ids, points, period):
    index = freq_ids[:, None] % period * points[None, :] % period
    angle = 2.0 * math.pi / period * index.astype(jnp.float32)
    return (jnp.cos(angle), jnp.sin(angle))

def build_tables():
    freq_ids = jnp.arange(FREQ, dtype=jnp.int32) - FREQ // 2
    win_len = ROWS + 2 * HALO
    row_cos, row_sin = phase_pair(freq_ids, jnp.arange(win_len, dtype=jnp.int32), win_len)
    forward_rows = (jnp.concatenate([row_cos, -row_sin], 0) / win_len).astype(jnp.bfloat16)
    col_cos, col_sin = phase_pair(freq_ids, jnp.arange(COLS, dtype=jnp.int32), COLS)
    real_part = jnp.concatenate([col_cos.T, -col_sin.T], 1) / COLS
    imag_part = jnp.concatenate([col_sin.T, col_cos.T], 1) / COLS
    forward_cols = jnp.stack([real_part, imag_part], 0).astype(jnp.bfloat16)
    inverse_cols = jnp.concatenate([jnp.concatenate([col_cos, col_sin], 1), jnp.concatenate([-col_sin, col_cos], 1)], 0).astype(jnp.bfloat16)
    inner_cos, inner_sin = phase_pair(freq_ids, jnp.arange(ROWS, dtype=jnp.int32) + HALO, win_len)
    inner_cos, inner_sin = (inner_cos.T, inner_sin.T)
    inverse_rows = jnp.stack([jnp.stack([inner_cos, -inner_sin], 1), jnp.stack([inner_sin, inner_cos], 1)], 0).astype(jnp.bfloat16)
    return (forward_rows, forward_cols, inverse_cols, inverse_rows)

def pupil_of(shifts):
    grid = jnp.arange(FREQ, dtype=jnp.int32) - FREQ // 2
    along_k = grid[None, :] + shifts[:, 0:1]
    along_l = grid[None, :] + shifts[:, 1:2]
    radius = FREQ // 4
    inside = along_k[:, :, None] * along_k[:, :, None] + along_l[:, None, :] * along_l[:, None, :] <= radius * radius
    pupil = inside.astype(jnp.float32)
    return jnp.concatenate([pupil, pupil], 2).astype(jnp.bfloat16)

def imaging(window, pupil, weights, tables, total_sources):
    forward_rows, forward_cols, inverse_cols, inverse_rows = tables
    count = pupil.shape[0]
    half = jnp.dot(forward_rows, window, preferred_element_type=jnp.float32).astype(jnp.bfloat16)
    spectrum = jnp.einsum('pkc,pcl->kl', half.reshape(2, FREQ, COLS).astype(jnp.float32), forward_cols.astype(jnp.float32)).astype(jnp.bfloat16)
    passed = pupil * spectrum[None]
    columns = jnp.dot(passed.reshape(count * FREQ, 2 * FREQ), inverse_cols, preferred_element_type=jnp.float32).astype(jnp.bfloat16)
    columns = columns.reshape(count, FREQ, 2, COLS)
    field = jnp.einsum('pxqk,skqc->spxc', inverse_rows.astype(jnp.float32), columns.astype(jnp.float32))
    scaled = weights / total_sources
    partial_sum = lax.optimization_barrier(jnp.sum(scaled[:, None, None, None] * field * field, axis=(0, 1)))
    return (field, partial_sum)

def adjoint_spectrum(field, d_int, pupil, weights, tables, total_sources):
    forward_rows, forward_cols, inverse_cols, inverse_rows = tables
    count = pupil.shape[0]
    coeff = 2.0 * weights / total_sources
    d_field = (coeff[:, None, None, None] * d_int[None, None] * field).astype(jnp.bfloat16)
    d_columns = jnp.einsum('pxqk,spxc->skqc', inverse_rows.astype(jnp.float32), d_field.astype(jnp.float32)).astype(jnp.bfloat16)
    d_passed = jnp.dot(d_columns.reshape(count * FREQ, 2 * COLS), inverse_cols.T, preferred_element_type=jnp.float32)
    d_passed = d_passed.reshape(count, FREQ, 2 * FREQ)
    return lax.optimization_barrier(jnp.sum(d_passed * pupil.astype(jnp.float32), axis=0))

def adjoint_window(d_spectrum, tables):
    forward_rows, forward_cols, inverse_cols, inverse_rows = tables
    d_half = jnp.einsum('kl,pcl->pkc', d_spectrum, forward_cols.astype(jnp.float32), precision=lax.Precision.HIGHEST)
    d_half = d_half.reshape(2 * FREQ, COLS)
    return jnp.dot(forward_rows.astype(jnp.float32).T, d_half, precision=lax.Precision.HIGHEST)

def reference(theta, target, source_shift, source_weight):
    tables = build_tables()
    pupil = pupil_of(source_shift)
    win_len = ROWS + 2 * HALO
    target_strips = target.astype(jnp.float32).reshape(N_STRIP, ROWS, COLS)
    resist = jnp.zeros((NR, COLS), jnp.float32)
    for iteration in range(ITERS):
        mask_now = jax.nn.sigmoid(theta)
        mask_low = mask_now.astype(jnp.bfloat16)
        padded = jnp.concatenate([mask_low[NR - HALO:], mask_low, mask_low[:HALO]], 0)

        def one_strip(operands):
            strip_id, target_rows = operands
            window = lax.dynamic_slice_in_dim(padded, (strip_id * ROWS).astype(jnp.int32), win_len, 0)
            field, intensity = imaging(window, pupil, source_weight, tables, SOURCES)
            resist_rows = jax.nn.sigmoid(steepness * (intensity - dose_level))
            d_int = 2.0 * (resist_rows - target_rows) * steepness * resist_rows * (1.0 - resist_rows)
            d_spectrum = adjoint_spectrum(field, d_int, pupil, source_weight, tables, SOURCES)
            return (resist_rows, adjoint_window(d_spectrum, tables))
        resist_all, windows = lax.map(one_strip, (jnp.arange(N_STRIP, dtype=jnp.int32), target_strips))
        center = windows[:, HALO:HALO + ROWS]
        from_next = jnp.roll(windows[:, :HALO], -1, axis=0)
        from_prev = jnp.roll(windows[:, HALO + ROWS:], 1, axis=0)
        gradient = center.at[:, :HALO].add(from_prev)
        gradient = gradient.at[:, ROWS - HALO:].add(from_next).reshape(NR, COLS)
        d_theta = gradient * mask_now * (1.0 - mask_now)
        squares = jnp.sum(d_theta * d_theta)
        theta = theta - step_size * d_theta * lax.rsqrt(squares / (NR * COLS) + epsilon)
        resist = resist_all.reshape(NR, COLS)
    return (theta, resist)
```

```python
import functools
import math

import jax
import jax.numpy as jnp
import numpy as np
from jax import lax
from jax.experimental import pallas as pl
from jax.experimental.pallas import tpu as pltpu
from jax.sharding import PartitionSpec as P

HALO = 64
FREQ = 128
ITERS = 2

steepness = 20.0
dose_level = 0.27
step_size = 1.0
epsilon = 1e-06

RADIUS = FREQ // 4
MAX_SHIFT = FREQ // 8
LOW = FREQ // 2 - RADIUS - MAX_SHIFT
KEEP = FREQ - LOW
ALIGN = 16
SPAN = 2 * RADIUS + ALIGN
VARIANTS = 2 * MAX_SHIFT // ALIGN + 1
SPLIT = 2
GROUP = 8


def shifted(array, axis, by):
    size = lax.axis_size(axis)
    return lax.ppermute(array, axis, [(i, (i + by) % size) for i in range(size)])


def partner(array):
    size = lax.axis_size("src")
    return lax.ppermute(array, "src", [(i, i ^ 1) for i in range(size)])


def phase_pair(freq_ids, points, period):
    index = freq_ids[:, None] % period * points[None, :] % period
    angle = np.float32(2.0 * math.pi / period) * index.astype(np.float32)
    return (np.cos(angle), np.sin(angle))


@functools.lru_cache(maxsize=None)
def build_tables(rows, cols):
    low = jnp.bfloat16
    freq_ids = np.arange(FREQ, dtype=np.int32) - FREQ // 2
    win_len = rows + 2 * HALO
    row_cos, row_sin = phase_pair(freq_ids, np.arange(win_len, dtype=np.int32), win_len)
    forward_rows = (np.concatenate([row_cos, -row_sin], 0) / np.float32(win_len)).astype(low)
    col_cos, col_sin = phase_pair(freq_ids, np.arange(cols, dtype=np.int32), cols)
    real_part = np.concatenate([col_cos.T, -col_sin.T], 1) / np.float32(cols)
    imag_part = np.concatenate([col_sin.T, col_cos.T], 1) / np.float32(cols)
    forward_cols = np.stack([real_part, imag_part], 0).astype(low)
    halves = []
    for part in range(SPLIT):
        at = slice(part * cols // SPLIT, (part + 1) * cols // SPLIT)
        halves.append(
            np.concatenate(
                [
                    np.concatenate([col_cos[:, at], col_sin[:, at]], 1),
                    np.concatenate([-col_sin[:, at], col_cos[:, at]], 1),
                ],
                0,
            )
        )
    inverse_cols = np.stack(halves, 0).astype(low)
    inner_cos, inner_sin = phase_pair(freq_ids, np.arange(rows, dtype=np.int32) + HALO, win_len)
    inner_cos, inner_sin = (inner_cos.T, inner_sin.T)
    inverse_rows = np.stack(
        [np.stack([inner_cos, -inner_sin], 1), np.stack([inner_sin, inner_cos], 1)], 0
    ).astype(low)
    windows = np.stack(
        [
            inverse_rows[:, :, :, LOW + v * ALIGN : LOW + v * ALIGN + SPAN].reshape(2 * rows, 2 * SPAN)
            for v in range(VARIANTS)
        ],
        0,
    )
    inverse_rows_t = inverse_rows.transpose(2, 3, 0, 1).reshape(2 * FREQ, 2 * rows)
    return (forward_rows, np.ascontiguousarray(forward_rows.T), forward_cols, inverse_cols, windows, np.ascontiguousarray(inverse_rows_t))


def dot(a, b):
    return jnp.dot(a, b, preferred_element_type=jnp.float32)


def dot_t(a, b):
    return lax.dot_general(a, b, (((1,), (1,)), ((), ())), preferred_element_type=jnp.float32)


def window_of(shift_ref, s):
    base = RADIUS + (FREQ // 2 - 2 * RADIUS) - shift_ref[s, 0]
    return pl.multiple_of(lax.shift_left(lax.shift_right_logical(base, 4), 4), ALIGN)


def image(mask, shift_ref, weight_ref, tables, target_ref, partial_ref, resist_ref, scratch, rows):
    fr_ref, fc_ref, gc_ref, grw_ref, grt_ref = tables
    spec_ref, pupil_ref, cols_ref, field_ref, dcols_ref, inten_ref, acc_ref = scratch
    sources = field_ref.shape[0]
    width = field_ref.shape[2]
    half = dot(fr_ref[...], mask).astype(jnp.bfloat16)
    spectrum = dot(half[:FREQ], fc_ref[0]) + dot(half[FREQ:], fc_ref[1])
    spec_ref[...] = spectrum.astype(jnp.bfloat16).astype(jnp.float32)
    inten_ref[...] = jnp.zeros_like(inten_ref)
    acc_ref[...] = jnp.zeros_like(acc_ref)

    def to_columns(g, carry):
        pieces = []
        for i in range(GROUP):
            s = g * GROUP + i
            base = window_of(shift_ref, s)
            along_k = lax.broadcasted_iota(jnp.int32, (SPAN, FREQ), 0) + (base - FREQ // 2 + shift_ref[s, 0])
            along_l = lax.broadcasted_iota(jnp.int32, (SPAN, FREQ), 1) + (shift_ref[s, 1] - FREQ // 2)
            inside = along_k * along_k + along_l * along_l <= RADIUS * RADIUS
            pupil = jnp.where(inside, 1.0, 0.0)
            pupil_ref[s] = pupil
            part = spec_ref[pl.ds(base, SPAN), :]
            pieces.append((part * jnp.concatenate([pupil, pupil], 1)).astype(jnp.bfloat16))
        out = dot(jnp.concatenate(pieces, 0), gc_ref[0]).astype(jnp.bfloat16)
        for i in range(GROUP):
            s = g * GROUP + i
            cols_ref[s, :SPAN, :] = out[i * SPAN : (i + 1) * SPAN, :width]
            cols_ref[s, SPAN:, :] = out[i * SPAN : (i + 1) * SPAN, width:]
        return carry

    lax.fori_loop(0, sources // GROUP, to_columns, 0)

    step = 4

    def to_field(g, carry):
        total = inten_ref[...]
        for i in range(step):
            s = g * step + i
            variant = lax.shift_right_logical(window_of(shift_ref, s) - LOW, 4)
            field = dot(grw_ref[variant], cols_ref[s])
            field_ref[s] = field
            scaled = weight_ref[s] * (1.0 / sources)
            total = total + scaled * (field[:rows] * field[:rows] + field[rows:] * field[rows:])
        inten_ref[...] = total
        return carry

    lax.fori_loop(0, sources // step, to_field, 0)

    resist = jax.nn.sigmoid(steepness * (inten_ref[...] - dose_level))
    if resist_ref is not None:
        resist_ref[...] = resist
    goal = target_ref[...].astype(jnp.float32)
    inten_ref[...] = 2.0 * (resist - goal) * steepness * resist * (1.0 - resist)

    def to_d_columns(g, carry):
        d_int = inten_ref[...]
        for i in range(step):
            s = g * step + i
            base = window_of(shift_ref, s)
            scale = d_int * (2.0 * weight_ref[s] * (1.0 / sources))
            d_field = (field_ref[s] * jnp.concatenate([scale, scale], 0)).astype(jnp.bfloat16)
            table = jnp.concatenate([grt_ref[pl.ds(base, SPAN), :], grt_ref[pl.ds(base + FREQ, SPAN), :]], 0)
            d_cols = dot(table, d_field).astype(jnp.bfloat16)
            dcols_ref[s, :, :width] = d_cols[:SPAN]
            dcols_ref[s, :, width:] = d_cols[SPAN:]
        return carry

    lax.fori_loop(0, sources // step, to_d_columns, 0)

    def to_d_spectrum(g, carry):
        d_cols = dcols_ref[pl.ds(g * GROUP, GROUP)].reshape(GROUP * SPAN, 2 * width)
        d_passed = dot_t(d_cols, gc_ref[0])
        for i in range(GROUP):
            s = g * GROUP + i
            base = window_of(shift_ref, s)
            pupil = pupil_ref[s]
            part = d_passed[i * SPAN : (i + 1) * SPAN] * jnp.concatenate([pupil, pupil], 1)
            acc_ref[pl.ds(base, SPAN), :] = acc_ref[pl.ds(base, SPAN), :] + part
        return carry

    lax.fori_loop(0, sources // GROUP, to_d_spectrum, 0)
    partial_ref[...] = acc_ref[LOW:, :].astype(partial_ref.dtype)


def d_windows(mine, other, fc_ref, frt_ref, dhi_ref, dlo_ref, field_ref):
    count = len(mine)
    width = field_ref.shape[2]
    zero = jnp.zeros((LOW, 2 * FREQ), jnp.bfloat16)
    for o in range(count):
        total = mine[o][...].astype(jnp.float32) + other[o][...].astype(jnp.float32)
        high = total.astype(jnp.bfloat16)
        rest = (total - high.astype(jnp.float32)).astype(jnp.bfloat16)
        high = jnp.concatenate([zero, high], 0)
        rest = jnp.concatenate([zero, rest], 0)
        for p in range(2):
            d_half = dot_t(high, fc_ref[p]) + dot_t(rest, fc_ref[p])
            d_high = d_half.astype(jnp.bfloat16)
            dhi_ref[o, p * FREQ : (p + 1) * FREQ, :] = d_high
            dlo_ref[o, p * FREQ : (p + 1) * FREQ, :] = (d_half - d_high.astype(jnp.float32)).astype(jnp.bfloat16)
    for o in range(count):
        d_win = dot(frt_ref[...], dhi_ref[o]) + dot(frt_ref[...], dlo_ref[o])
        for h in range(SPLIT):
            field_ref[SPLIT * o + h] = d_win[:, h * width : (h + 1) * width]


def d_block(field_ref, i, count, rows):
    prev = (i - 1) % count
    return jnp.concatenate(
        [field_ref[SPLIT * i + h, :rows, :] + field_ref[SPLIT * prev + h, rows:, :] for h in range(SPLIT)], 1
    )


def put_block(field_ref, i, rows, value):
    width = field_ref.shape[2]
    for h in range(SPLIT):
        field_ref[SPLIT * i + h, :rows, :] = value[:, h * width : (h + 1) * width]


def get_block(field_ref, i, rows):
    return jnp.concatenate([field_ref[SPLIT * i + h, :rows, :] for h in range(SPLIT)], 1)


def gradients(blocks, field_ref, rows, cols):
    count = len(blocks)
    squares = jnp.zeros((1, 1), jnp.float32)
    for i, block in enumerate(blocks):
        m = jax.nn.sigmoid(block())
        d_theta = d_block(field_ref, i, count, rows) * m * (1.0 - m)
        put_block(field_ref, i, rows, d_theta)
        squares = squares + jnp.sum(d_theta * d_theta, axis=(0, 1), keepdims=True)
    return step_size * lax.rsqrt(squares / (rows * count * cols) + epsilon)


def blocks_of(prev_ref, own_ref, next_ref, rest_refs, rows):
    pieces = [(prev_ref, 0), (own_ref, 0), (own_ref, HALO), (next_ref, 0)]
    for ref in rest_refs:
        pieces += [(ref, at) for at in range(0, ref.shape[0], HALO)]
    per = rows // HALO

    def load(i):
        return jnp.concatenate(
            [ref[at : at + HALO, :].astype(jnp.float32) for ref, at in pieces[i * per : (i + 1) * per]], 0
        )

    return [functools.partial(load, i) for i in range(len(pieces) // per)]


def first_kernel(half_ref, shift_ref, weight_ref, prev_ref, own_ref, next_ref, target_ref, fr_ref, frt_ref, fc_ref, gc_ref, grw_ref, grt_ref, partial_ref, *scratch):
    rows = own_ref.shape[0]
    theta = jnp.concatenate([prev_ref[...], own_ref[...], next_ref[...]], 0)
    mask = jax.nn.sigmoid(theta).astype(jnp.bfloat16)
    image(mask, shift_ref, weight_ref, (fr_ref, fc_ref, gc_ref, grw_ref, grt_ref), target_ref, partial_ref, None, scratch, rows)


def later_kernel(count, rests, *refs):
    half_ref, shift_ref, weight_ref = refs[:3]
    refs = refs[3:]
    mine, other, refs = refs[:count], refs[count : 2 * count], refs[2 * count :]
    prev_ref, own_ref, next_ref = refs[:3]
    rest_refs, refs = refs[3 : 3 + rests], refs[3 + rests :]
    target_ref, fr_ref, frt_ref, fc_ref, gc_ref, grw_ref, grt_ref = refs[:7]
    partial_ref, resist_ref, prev_out, own_out, next_out, rest_out = refs[7:13]
    scratch, (dhi_ref, dlo_ref) = refs[13:20], refs[20:]
    field_ref = scratch[3]
    rows, cols = own_ref.shape
    d_windows(mine, other, fc_ref, frt_ref, dhi_ref, dlo_ref, field_ref)
    blocks = blocks_of(prev_ref, own_ref, next_ref, rest_refs, rows)
    factor = gradients(blocks, field_ref, rows, cols)
    masks = []
    for i, block in enumerate(blocks):
        theta = block() - get_block(field_ref, i, rows) * factor
        if i == 0:
            prev_out[...] = theta[:HALO]
            own_out[:HALO, :] = theta[HALO:]
        elif i == 1:
            own_out[HALO:, :] = theta[: rows - HALO]
            next_out[...] = theta[rows - HALO :]
        else:
            rest_out[(i - 2) * rows : (i - 1) * rows, :] = theta
        if i < 2:
            masks.append(jax.nn.sigmoid(theta).astype(jnp.bfloat16))
    image(jnp.concatenate(masks, 0), shift_ref, weight_ref, (fr_ref, fc_ref, gc_ref, grw_ref, grt_ref), target_ref, partial_ref, resist_ref, scratch, rows)


def last_kernel(count, rests, *refs):
    half_ref = refs[0]
    refs = refs[1:]
    mine, other, refs = refs[:count], refs[count : 2 * count], refs[2 * count :]
    prev_ref, own_ref, next_ref = refs[:3]
    rest_refs, refs = refs[3 : 3 + rests], refs[3 + rests :]
    fc_ref, frt_ref, resist_ref, resist_other, theta_out, resist_out, field_ref, dhi_ref, dlo_ref = refs
    rows, cols = own_ref.shape
    width = resist_ref.shape[1]
    d_windows(mine, other, fc_ref, frt_ref, dhi_ref, dlo_ref, field_ref)
    blocks = blocks_of(prev_ref, own_ref, next_ref, rest_refs, rows)
    factor = gradients(blocks, field_ref, rows, cols)
    d_own = jnp.concatenate([get_block(field_ref, 0, rows)[HALO:], get_block(field_ref, 1, rows)[: rows - HALO]], 0)
    theta_out[...] = own_ref[...] - d_own * factor
    first = half_ref[0] == 0
    resist_out[:, :width] = jnp.where(first, resist_ref[...], resist_other[...])
    resist_out[:, width:] = jnp.where(first, resist_other[...], resist_ref[...])


def per_device(theta, target, source_shift, source_weight):
    rows, cols = theta.shape
    count = lax.axis_size("strip")
    width = cols // SPLIT
    sources = source_weight.shape[0] * lax.axis_size("src")
    half = (lax.axis_index("src") % SPLIT).astype(jnp.int32).reshape(1)
    forward_rows, forward_rows_t, forward_cols, inverse_cols, windows, inverse_rows_t = [
        jnp.asarray(t) for t in build_tables(rows, cols)
    ]

    packed = jnp.concatenate([source_shift.astype(jnp.float32), source_weight[:, None]], 1)
    prev_rows = shifted(theta[rows - HALO :], "strip", 1)
    next_rows = shifted(theta[:HALO], "strip", -1)
    packed = lax.all_gather(packed, "src", axis=0, tiled=True)
    shifts = packed[:, :2].astype(jnp.int32)
    weights = packed[:, 2]

    low = theta.astype(jnp.bfloat16)
    rest = [shifted(low[rows - HALO :], "strip", -1)]
    rest += [shifted(low, "strip", -o) for o in range(2, count - 1)]
    rest += [shifted(low[:HALO], "strip", 1)]

    vmem = pl.BlockSpec(memory_space=pltpu.VMEM)
    smem = pl.BlockSpec(memory_space=pltpu.SMEM)

    def full(shape):
        return pl.BlockSpec(shape, lambda i, at: (0,) * len(shape))

    def column_half(shape):
        return pl.BlockSpec(shape, lambda i, at: (0, at[0]))

    cut = pl.BlockSpec((1, 2 * FREQ, SPLIT * width), lambda i, at: (at[0], 0, 0))
    table_specs = [
        full(forward_rows.shape), full(forward_rows_t.shape), full(forward_cols.shape), cut,
        full(windows.shape), full(inverse_rows_t.shape),
    ]
    tables = (forward_rows, forward_rows_t, forward_cols, inverse_cols, windows, inverse_rows_t)
    image_scratch = [
        pltpu.VMEM((FREQ, 2 * FREQ), jnp.float32),
        pltpu.VMEM((sources, SPAN, FREQ), jnp.float32),
        pltpu.VMEM((sources, 2 * SPAN, width), jnp.bfloat16),
        pltpu.VMEM((sources, 2 * rows, width), jnp.float32),
        pltpu.VMEM((sources, SPAN, 2 * width), jnp.bfloat16),
        pltpu.VMEM((rows, width), jnp.float32),
        pltpu.VMEM((FREQ, 2 * FREQ), jnp.float32),
    ]
    adjoint_scratch = [pltpu.VMEM((count, 2 * FREQ, cols), jnp.bfloat16)] * 2
    params = pltpu.CompilerParams(vmem_limit_bytes=60 << 20)
    cost = pl.CostEstimate(flops=6 << 30, bytes_accessed=4 << 20, transcendentals=1 << 20)
    small_cost = pl.CostEstimate(flops=1 << 30, bytes_accessed=4 << 20, transcendentals=1 << 20)

    def call(kernel, in_specs, out_shapes, out_specs, scratch, args, estimate, name):
        return pl.pallas_call(
            kernel,
            out_shape=out_shapes,
            grid_spec=pltpu.PrefetchScalarGridSpec(
                num_scalar_prefetch=1, grid=(1,), in_specs=in_specs, out_specs=out_specs, scratch_shapes=scratch
            ),
            compiler_params=params,
            cost_estimate=estimate,
            name=name,
        )(half, *args)

    f32 = jnp.float32
    partial_shape = jax.ShapeDtypeStruct((KEEP, 2 * FREQ), f32)
    final_shape = jax.ShapeDtypeStruct((KEEP, 2 * FREQ), jnp.bfloat16)
    state = [prev_rows, theta, next_rows]
    (partial,) = call(
        first_kernel,
        [smem, smem] + [full(a.shape) for a in state] + [column_half((rows, width))] + table_specs,
        [partial_shape],
        [full(partial_shape.shape)],
        image_scratch,
        [shifts, weights, *state, target, *tables],
        cost,
        "first_image",
    )
    for later in range(1, ITERS):
        mine = [partial] + [shifted(partial, "strip", -o) for o in range(1, count)]
        other = [partner(a) for a in mine]
        args = [*mine, *other, *state, *rest]
        outs = [
            final_shape if later == ITERS - 1 else partial_shape,
            jax.ShapeDtypeStruct((rows, width), f32),
            *[jax.ShapeDtypeStruct(a.shape, f32) for a in state],
            jax.ShapeDtypeStruct(((count - 2) * rows, cols), f32),
        ]
        partial, resist, *moved = call(
            functools.partial(later_kernel, count, len(rest)),
            [smem, smem] + [full(a.shape) for a in args] + [column_half((rows, width))] + table_specs,
            outs,
            [full(a.shape) for a in outs],
            image_scratch + adjoint_scratch,
            [shifts, weights, *args, target, *tables],
            cost,
            "later_image",
        )
        state, rest = moved[:3], moved[3:]
    mine = [partial] + [shifted(partial, "strip", -o) for o in range(1, count)]
    other = [partner(a) for a in mine]
    resist_other = partner(resist)
    args = [*mine, *other, *state, *rest, forward_cols, forward_rows_t, resist, resist_other]
    outs = [jax.ShapeDtypeStruct((rows, cols), f32)] * 2
    theta, resist = call(
        functools.partial(last_kernel, count, len(rest)),
        [full(a.shape) for a in args],
        outs,
        [full(a.shape) for a in outs],
        [pltpu.VMEM((SPLIT * count, 2 * rows, width), f32)] + adjoint_scratch,
        args,
        small_cost,
        "last_step",
    )
    return (theta, resist)


def solution(mesh):
    return jax.shard_map(
        per_device,
        mesh=mesh,
        in_specs=(P(("band", "strip"), None), P(("band", "strip"), None), P("src", None), P("src")),
        out_specs=(P(("band", "strip"), None), P(("band", "strip"), None)),
        check_vma=False,
    )
```

```python
import functools
import math

import jax
import jax.numpy as jnp
import numpy as np
from jax import lax
from jax.experimental import pallas as pl
from jax.experimental.pallas import tpu as pltpu
from jax.sharding import PartitionSpec as P

HALO = 64
FREQ = 128
ITERS = 2

steepness = 20.0
dose_level = 0.27
step_size = 1.0
epsilon = 1e-06

RADIUS = FREQ // 4
MAX_SHIFT = FREQ // 8
LOW = FREQ // 2 - RADIUS - MAX_SHIFT
KEEP = FREQ - LOW
ALIGN = 16
SPAN = 2 * RADIUS + ALIGN
VARIANTS = 2 * MAX_SHIFT // ALIGN + 1
SPLIT = 2
GROUP = 16
STEP = 8


def shifted(array, axis, by):
    size = lax.axis_size(axis)
    return lax.ppermute(array, axis, [(i, (i + by) % size) for i in range(size)])


def partner(array):
    size = lax.axis_size("src")
    return lax.ppermute(array, "src", [(i, i ^ 1) for i in range(size)])


def phase_pair(freq_ids, points, period):
    index = freq_ids[:, None] % period * points[None, :] % period
    angle = np.float32(2.0 * math.pi / period) * index.astype(np.float32)
    return (np.cos(angle), np.sin(angle))


@functools.lru_cache(maxsize=None)
def build_tables(rows, cols):
    low = jnp.bfloat16
    freq_ids = np.arange(FREQ, dtype=np.int32) - FREQ // 2
    win_len = rows + 2 * HALO
    row_cos, row_sin = phase_pair(freq_ids, np.arange(win_len, dtype=np.int32), win_len)
    forward_rows = (np.concatenate([row_cos, -row_sin], 0) / np.float32(win_len)).astype(low)
    col_cos, col_sin = phase_pair(freq_ids, np.arange(cols, dtype=np.int32), cols)
    real_part = np.concatenate([col_cos.T, -col_sin.T], 1) / np.float32(cols)
    imag_part = np.concatenate([col_sin.T, col_cos.T], 1) / np.float32(cols)
    forward_cols = np.stack([real_part, imag_part], 0).astype(low)
    halves = []
    for part in range(SPLIT):
        at = slice(part * cols // SPLIT, (part + 1) * cols // SPLIT)
        halves.append(
            np.concatenate(
                [
                    np.concatenate([col_cos[:, at], col_sin[:, at]], 1),
                    np.concatenate([-col_sin[:, at], col_cos[:, at]], 1),
                ],
                0,
            )
        )
    inverse_cols = np.stack(halves, 0).astype(low)
    inner_cos, inner_sin = phase_pair(freq_ids, np.arange(rows, dtype=np.int32) + HALO, win_len)
    inner_cos, inner_sin = (inner_cos.T, inner_sin.T)
    inverse_rows = np.stack(
        [np.stack([inner_cos, -inner_sin], 1), np.stack([inner_sin, inner_cos], 1)], 0
    ).astype(low)
    windows = np.stack(
        [
            inverse_rows[:, :, :, LOW + v * ALIGN : LOW + v * ALIGN + SPAN].reshape(2 * rows, 2 * SPAN)
            for v in range(VARIANTS)
        ],
        0,
    )
    inverse_rows_t = inverse_rows.transpose(2, 3, 0, 1).reshape(2 * FREQ, 2 * rows)
    return (forward_rows, np.ascontiguousarray(forward_rows.T), forward_cols, inverse_cols, windows, np.ascontiguousarray(inverse_rows_t))


def dot(a, b):
    return jnp.dot(a, b, preferred_element_type=jnp.float32)


def dot_t(a, b):
    return lax.dot_general(a, b, (((1,), (1,)), ((), ())), preferred_element_type=jnp.float32)


def read_sources(packs, at_ref, weight_ref):
    per = packs[0].shape[0] // 3
    for d, pack in enumerate(packs):
        for i in range(per):
            s = d * per + i
            along_k = pack[2 * i].astype(jnp.int32)
            first = FREQ // 2 - RADIUS - along_k
            at_ref[0, s] = first - lax.rem(first, ALIGN)
            at_ref[1, s] = along_k - FREQ // 2
            at_ref[2, s] = pack[2 * i + 1].astype(jnp.int32) - FREQ // 2
            weight_ref[s] = pack[2 * per + i]


def window_of(at_ref, s):
    return pl.multiple_of(at_ref[0, s], ALIGN)


def image(mask, shift_ref, weight_ref, tables, target_ref, partial_ref, resist_ref, scratch, rows):
    fr_ref, fc_ref, gc_ref, grw_ref, grt_ref = tables
    spec_ref, pupil_ref, cols_ref, field_ref, dcols_ref, inten_ref, acc_ref = scratch
    sources = field_ref.shape[0]
    width = field_ref.shape[2]
    half = dot(fr_ref[...], mask).astype(jnp.bfloat16)
    spectrum = dot(half[:FREQ], fc_ref[0]) + dot(half[FREQ:], fc_ref[1])
    spec_ref[...] = spectrum.astype(jnp.bfloat16).astype(jnp.float32)
    inten_ref[...] = jnp.zeros_like(inten_ref)
    acc_ref[...] = jnp.zeros_like(acc_ref)

    def to_columns(g, carry):
        pieces = []
        for i in range(GROUP):
            s = g * GROUP + i
            base = window_of(shift_ref, s)
            along_k = lax.broadcasted_iota(jnp.int32, (SPAN, FREQ), 0) + (base + shift_ref[1, s])
            along_l = lax.broadcasted_iota(jnp.int32, (SPAN, FREQ), 1) + shift_ref[2, s]
            inside = along_k * along_k + along_l * along_l <= RADIUS * RADIUS
            pupil = jnp.where(inside, 1.0, 0.0)
            pupil_ref[s] = pupil
            part = spec_ref[pl.ds(base, SPAN), :]
            pieces.append((part * jnp.concatenate([pupil, pupil], 1)).astype(jnp.bfloat16))
        out = dot(jnp.concatenate(pieces, 0), gc_ref[...]).astype(jnp.bfloat16)
        for i in range(GROUP):
            s = g * GROUP + i
            cols_ref[s, :SPAN, :] = out[i * SPAN : (i + 1) * SPAN, :width]
            cols_ref[s, SPAN:, :] = out[i * SPAN : (i + 1) * SPAN, width:]
        return carry

    lax.fori_loop(0, sources // GROUP, to_columns, 0)

    def to_field(g, carry):
        total = inten_ref[...]
        for i in range(STEP):
            s = g * STEP + i
            variant = lax.div(shift_ref[0, s] - LOW, ALIGN)
            field = dot(grw_ref[variant], cols_ref[s])
            field_ref[s] = field
            scaled = weight_ref[s] * (1.0 / sources)
            total = total + scaled * (field[:rows] * field[:rows] + field[rows:] * field[rows:])
        inten_ref[...] = total
        return carry

    lax.fori_loop(0, sources // STEP, to_field, 0)

    resist = jax.nn.sigmoid(steepness * (inten_ref[...] - dose_level))
    if resist_ref is not None:
        resist_ref[...] = resist
    goal = target_ref[...].astype(jnp.float32)
    inten_ref[...] = 2.0 * (resist - goal) * steepness * resist * (1.0 - resist)

    def to_d_columns(g, carry):
        d_int = inten_ref[...]
        for i in range(STEP):
            s = g * STEP + i
            base = window_of(shift_ref, s)
            scale = d_int * (2.0 * weight_ref[s] * (1.0 / sources))
            d_field = (field_ref[s] * jnp.concatenate([scale, scale], 0)).astype(jnp.bfloat16)
            table = jnp.concatenate([grt_ref[pl.ds(base, SPAN), :], grt_ref[pl.ds(base + FREQ, SPAN), :]], 0)
            d_cols = dot(table, d_field).astype(jnp.bfloat16)
            dcols_ref[s, :, :width] = d_cols[:SPAN]
            dcols_ref[s, :, width:] = d_cols[SPAN:]
        return carry

    lax.fori_loop(0, sources // STEP, to_d_columns, 0)

    def to_d_spectrum(g, carry):
        d_cols = dcols_ref[pl.ds(g * GROUP, GROUP)].reshape(GROUP * SPAN, 2 * width)
        d_passed = dot_t(d_cols, gc_ref[...])
        for i in range(GROUP):
            s = g * GROUP + i
            base = window_of(shift_ref, s)
            pupil = pupil_ref[s]
            part = d_passed[i * SPAN : (i + 1) * SPAN] * jnp.concatenate([pupil, pupil], 1)
            acc_ref[pl.ds(base, SPAN), :] = acc_ref[pl.ds(base, SPAN), :] + part
        return carry

    lax.fori_loop(0, sources // GROUP, to_d_spectrum, 0)
    partial_ref[...] = acc_ref[LOW:, :].astype(partial_ref.dtype)


def d_windows(sums, half, fc_ref, frt_ref, dhi_ref, dlo_ref, field_ref, count):
    width = field_ref.shape[2]
    zero = jnp.zeros((LOW, 2 * FREQ), jnp.bfloat16)

    def one(o, total):
        total = total.astype(jnp.float32)
        high = total.astype(jnp.bfloat16)
        rest = (total - high.astype(jnp.float32)).astype(jnp.bfloat16)
        high = jnp.concatenate([zero, high], 0)
        rest = jnp.concatenate([zero, rest], 0)
        for p in range(2):
            d_half = dot_t(high, fc_ref[p]) + dot_t(rest, fc_ref[p])
            d_high = d_half.astype(jnp.bfloat16)
            dhi_ref[o, p * FREQ : (p + 1) * FREQ, :] = d_high
            dlo_ref[o, p * FREQ : (p + 1) * FREQ, :] = (d_half - d_high.astype(jnp.float32)).astype(jnp.bfloat16)

    one(0, sums[0][...])
    for (low, high), mine, other in zip(pairs_of(count), sums[1::2], sums[2::2]):
        if low == high:
            first = jnp.where(half == 0, mine[...], other[...])
            second = jnp.where(half == 0, other[...], mine[...])
            one(low, jnp.concatenate([first, second], 0))
        else:
            one(jnp.where(half == 0, low, high), mine[...])
            one(jnp.where(half == 0, high, low), other[...])
    for o in range(count):
        d_win = dot(frt_ref[...], dhi_ref[o]) + dot(frt_ref[...], dlo_ref[o])
        for h in range(SPLIT):
            field_ref[SPLIT * o + h] = d_win[:, h * width : (h + 1) * width]


def d_block(field_ref, i, count, rows):
    prev = (i - 1) % count
    return jnp.concatenate(
        [field_ref[SPLIT * i + h, :rows, :] + field_ref[SPLIT * prev + h, rows:, :] for h in range(SPLIT)], 1
    )


def put_block(field_ref, i, rows, value):
    width = field_ref.shape[2]
    for h in range(SPLIT):
        field_ref[SPLIT * i + h, :rows, :] = value[:, h * width : (h + 1) * width]


def get_block(field_ref, i, rows):
    return jnp.concatenate([field_ref[SPLIT * i + h, :rows, :] for h in range(SPLIT)], 1)


def gradients(blocks, field_ref, rows, cols):
    count = len(blocks)
    squares = jnp.zeros((1, 1), jnp.float32)
    for i, block in enumerate(blocks):
        m = jax.nn.sigmoid(block())
        d_theta = d_block(field_ref, i, count, rows) * m * (1.0 - m)
        put_block(field_ref, i, rows, d_theta)
        squares = squares + jnp.sum(d_theta * d_theta, axis=(0, 1), keepdims=True)
    return step_size * lax.rsqrt(squares / (rows * count * cols) + epsilon)


def blocks_of(state_refs, rows):
    pieces = [(ref, at) for ref in state_refs for at in range(0, ref.shape[0], HALO)]
    per = rows // HALO

    def load(i):
        return jnp.concatenate(
            [ref[at : at + HALO, :].astype(jnp.float32) for ref, at in pieces[i * per : (i + 1) * per]], 0
        )

    return [functools.partial(load, i) for i in range(len(pieces) // per)]


def first_kernel(n_packs, *refs):
    half_ref, packs, refs = refs[0], refs[1 : 1 + n_packs], refs[1 + n_packs :]
    mine_ref, other_ref, own_ref, target_ref = refs[:4]
    fr_ref, fc_ref, gc_ref, grw_ref, grt_ref, partial_ref, at_ref, weight_ref = refs[4:12]
    scratch = refs[12:]
    rows = own_ref.shape[0]
    read_sources(packs, at_ref, weight_ref)
    first = half_ref[0] == 0
    mine, other = mine_ref[...], other_ref[...]
    theta = jnp.concatenate([jnp.where(first, mine, other), own_ref[...], jnp.where(first, other, mine)], 0)
    mask = jax.nn.sigmoid(theta).astype(jnp.bfloat16)
    image(mask, at_ref, weight_ref, (fr_ref, fc_ref, gc_ref, grw_ref, grt_ref), target_ref, partial_ref, None, scratch, rows)


def later_kernel(count, n_packs, n_sums, n_state, gathered, *refs):
    half_ref, packs, refs = refs[0], refs[1 : 1 + n_packs], refs[1 + n_packs :]
    sums, state, refs = refs[:n_sums], refs[n_sums : n_sums + n_state], refs[n_sums + n_state :]
    target_ref, fr_ref, frt_ref, fc_ref, gc_ref, grw_ref, grt_ref = refs[:7]
    partial_ref, resist_ref, window_out, rest_out = refs[7:11]
    at_ref, weight_ref = refs[11:13]
    scratch, (dhi_ref, dlo_ref, band_ref) = refs[13:20], refs[20:]
    field_ref = scratch[3]
    rows, cols = window_out.shape[0] // 2, window_out.shape[1]
    half = half_ref[0]
    read_sources(packs, at_ref, weight_ref)
    if gathered:
        blocks = blocks_of(state, rows)
    else:
        place_state(state, half, band_ref, count, rows)
        blocks = blocks_of([band_ref], rows)
    d_windows(sums, half, fc_ref, frt_ref, dhi_ref, dlo_ref, field_ref, count)
    factor = gradients(blocks, field_ref, rows, cols)
    masks = []
    for i, block in enumerate(blocks):
        theta = block() - get_block(field_ref, i, rows) * factor
        if i < 2:
            window_out[i * rows : (i + 1) * rows, :] = theta
            masks.append(jax.nn.sigmoid(theta).astype(jnp.bfloat16))
        else:
            rest_out[(i - 2) * rows : (i - 1) * rows, :] = theta
    image(jnp.concatenate(masks, 0), at_ref, weight_ref, (fr_ref, fc_ref, gc_ref, grw_ref, grt_ref), target_ref, partial_ref, resist_ref, scratch, rows)


def place_state(state, half, band_ref, count, rows):
    own_ref, pieces = state[0], state[1:]
    band_ref[HALO : HALO + rows, :] = own_ref[...]
    whole = count * rows

    def put(first_row, second_row, mine, other):
        a = pl.multiple_of(jnp.where(half == 0, first_row, second_row), HALO)
        b = pl.multiple_of(jnp.where(half == 0, second_row, first_row), HALO)
        band_ref[pl.ds(a, HALO), :] = mine[...].astype(jnp.float32)
        band_ref[pl.ds(b, HALO), :] = other[...].astype(jnp.float32)

    put(0, HALO + rows, pieces[0], pieces[1])
    put(2 * rows, whole - HALO, pieces[2], pieces[3])
    for k, o in enumerate(range(2, count - 1)):
        put(HALO + o * rows, 2 * HALO + o * rows, pieces[4 + 2 * k], pieces[5 + 2 * k])


def last_kernel(count, n_sums, *refs):
    half_ref, refs = refs[0], refs[1:]
    sums, state, refs = refs[:n_sums], refs[n_sums : n_sums + 2], refs[n_sums + 2 :]
    fc_ref, frt_ref, resist_ref, resist_other, theta_out, resist_out, field_ref, dhi_ref, dlo_ref = refs
    rows, cols = theta_out.shape
    width = resist_ref.shape[1]
    half = half_ref[0]
    d_windows(sums, half, fc_ref, frt_ref, dhi_ref, dlo_ref, field_ref, count)
    factor = gradients(blocks_of(state, rows), field_ref, rows, cols)
    d_own = jnp.concatenate([get_block(field_ref, 0, rows)[HALO:], get_block(field_ref, 1, rows)[: rows - HALO]], 0)
    theta_out[...] = state[0][HALO : HALO + rows, :] - d_own * factor
    first = half == 0
    resist_out[:, :width] = jnp.where(first, resist_ref[...], resist_other[...])
    resist_out[:, width:] = jnp.where(first, resist_other[...], resist_ref[...])


def pairs_of(count):
    return [(o, count - o) for o in range(1, (count + 1) // 2)] + [(count // 2, count // 2)] * (count % 2 == 0)


def fetch(array, low, high):
    strips, size = lax.axis_size("strip"), lax.axis_size("src")
    steps = [
        (z * size + s, (z - (high if s % SPLIT else low)) % strips * size + s)
        for z in range(strips)
        for s in range(size)
    ]
    return lax.ppermute(array, ("strip", "src"), steps)


def exchange(partial, half, dtype):
    total = (partial + partner(partial)).astype(dtype)
    rows = total.shape[0] // 2
    sums = [total]
    for low, high in pairs_of(lax.axis_size("strip")):
        send = total
        if low == high:
            send = jnp.where(half == 0, total[:rows], total[rows:])
        mine = fetch(send, low, high)
        sums += [mine, partner(mine)]
    return sums


def per_device(theta, target, source_shift, source_weight):
    rows, cols = theta.shape
    count = lax.axis_size("strip")
    n_src = lax.axis_size("src")
    width = cols // SPLIT
    sources = source_weight.shape[0] * n_src
    half = (lax.axis_index("src") % SPLIT).astype(jnp.int32)
    forward_rows, forward_rows_t, forward_cols, inverse_cols, windows, inverse_rows_t = [
        jnp.asarray(t) for t in build_tables(rows, cols)
    ]
    inverse_cols = lax.dynamic_index_in_dim(inverse_cols, half, 0, keepdims=False)
    target = lax.dynamic_slice_in_dim(target, half * width, width, 1)

    even = half == 0
    head, tail = theta[:HALO], theta[rows - HALO :]
    mine = fetch(jnp.where(even, tail, head), count - 1, 1)
    pack = jnp.concatenate([source_shift.reshape(-1).astype(jnp.float32), source_weight])
    packs = [pack] + [shifted(pack, "src", k) for k in range(1, n_src)]
    pieces = [mine, partner(mine)]
    low = jnp.where(even, tail, head).astype(jnp.bfloat16)
    mine = fetch(low, 1, count - 1)
    pieces += [mine, partner(mine)]
    low = jnp.where(even, head, tail).astype(jnp.bfloat16)
    for o in range(2, count - 1):
        mine = fetch(low, o, o)
        pieces += [mine, partner(mine)]

    vmem = pl.BlockSpec(memory_space=pltpu.VMEM)
    smem = pl.BlockSpec(memory_space=pltpu.SMEM)
    f32 = jnp.float32
    source_scratch = [pltpu.SMEM((3, sources), jnp.int32), pltpu.SMEM((sources,), f32)]
    image_scratch = [
        pltpu.VMEM((FREQ, 2 * FREQ), f32),
        pltpu.VMEM((sources, SPAN, FREQ), f32),
        pltpu.VMEM((sources, 2 * SPAN, width), jnp.bfloat16),
        pltpu.VMEM((sources, 2 * rows, width), f32),
        pltpu.VMEM((sources, SPAN, 2 * width), jnp.bfloat16),
        pltpu.VMEM((rows, width), f32),
        pltpu.VMEM((FREQ, 2 * FREQ), f32),
    ]
    adjoint_scratch = [pltpu.VMEM((count, 2 * FREQ, cols), jnp.bfloat16)] * 2
    band_scratch = [pltpu.VMEM((count * rows, cols), f32)]

    def call(kernel, n_smem, args, outs, scratch, flops, name):
        held = sum(math.prod(a.shape) * a.dtype.itemsize for a in [*args, *outs])
        held += sum(math.prod(a.shape) * jnp.dtype(a.dtype).itemsize for a in scratch)
        return pl.pallas_call(
            kernel,
            out_shape=outs,
            in_specs=[smem] * n_smem + [vmem] * (len(args) - n_smem),
            out_specs=[vmem] * len(outs),
            scratch_shapes=scratch,
            compiler_params=pltpu.CompilerParams(vmem_limit_bytes=held + (6 << 20)),
            cost_estimate=pl.CostEstimate(flops=flops, bytes_accessed=4 << 20, transcendentals=1 << 20),
            name=name,
        )(*args)

    smalls = [half.reshape(1), *packs]
    partial_shape = jax.ShapeDtypeStruct((KEEP, 2 * FREQ), f32)
    image_tables = [forward_cols, inverse_cols, windows, inverse_rows_t]
    (partial,) = call(
        functools.partial(first_kernel, n_src),
        len(smalls),
        [*smalls, *pieces[:2], theta, target, forward_rows, *image_tables],
        [partial_shape],
        source_scratch + image_scratch,
        6 << 30,
        "first_image",
    )
    state, gathered = [theta, *pieces], False
    for _ in range(ITERS - 1):
        sums = exchange(partial, half, f32)
        partial, resist, *state = call(
            functools.partial(later_kernel, count, n_src, len(sums), len(state), gathered),
            len(smalls),
            [*smalls, *sums, *state, target, forward_rows, forward_rows_t, *image_tables],
            [
                partial_shape,
                jax.ShapeDtypeStruct((rows, width), f32),
                jax.ShapeDtypeStruct((2 * rows, cols), f32),
                jax.ShapeDtypeStruct(((count - 2) * rows, cols), f32),
            ],
            source_scratch + image_scratch + adjoint_scratch + band_scratch,
            6 << 30,
            "later_image",
        )
        gathered = True
    sums = exchange(partial, half, jnp.bfloat16)
    args = [half.reshape(1), *sums, *state, forward_cols, forward_rows_t, resist, partner(resist)]
    theta, resist = call(
        functools.partial(last_kernel, count, len(sums)),
        1,
        args,
        [jax.ShapeDtypeStruct((rows, cols), f32)] * 2,
        [pltpu.VMEM((SPLIT * count, 2 * rows, width), f32)] + adjoint_scratch,
        1 << 30,
        "last_step",
    )
    return (theta, resist)


def solution(mesh):
    return jax.shard_map(
        per_device,
        mesh=mesh,
        in_specs=(P(("band", "strip"), None), P(("band", "strip"), None), P("src", None), P("src")),
        out_specs=(P(("band", "strip"), None), P(("band", "strip"), None)),
        check_vma=False,
    )
```

```python
import functools
import math

import jax
import jax.numpy as jnp
import numpy as np
from jax import lax
from jax.experimental import pallas as pl
from jax.experimental.pallas import tpu as pltpu
from jax.sharding import PartitionSpec as P


HALO = 64
FREQ = 128
ITERS = 2

steepness = 20.0
dose_level = 0.27
step_size = 1.0
epsilon = 1e-06

RADIUS = FREQ // 4
MAX_SHIFT = FREQ // 8
LOW = FREQ // 2 - RADIUS - MAX_SHIFT
FOLD = -(-(RADIUS + MAX_SHIFT + 1) // 8) * 8
HALF = FREQ // 2
ALIGN = 16
SPAN = 2 * RADIUS + ALIGN
VARIANTS = 2 * MAX_SHIFT // ALIGN + 1
SPLIT = 2
GROUP = 8
STEP = 8


def shifted(array, axis, by):
    size = lax.axis_size(axis)
    return lax.ppermute(array, axis, [(i, (i + by) % size) for i in range(size)])


def partner(array):
    size = lax.axis_size("src")
    return lax.ppermute(array, "src", [(i, i ^ 1) for i in range(size)])


def phase_pair(freq_ids, points, period):
    index = freq_ids[:, None] % period * points[None, :] % period
    angle = np.float32(2.0 * math.pi / period) * index.astype(np.float32)
    return (np.cos(angle), np.sin(angle))


@functools.lru_cache(maxsize=None)
def build_tables(rows, cols):
    low = jnp.bfloat16
    freq_ids = np.arange(FREQ, dtype=np.int32) - FREQ // 2
    win_len = rows + 2 * HALO
    row_cos, row_sin = phase_pair(freq_ids, np.arange(win_len, dtype=np.int32), win_len)
    forward_rows = (np.concatenate([row_cos, -row_sin], 0) / np.float32(win_len)).astype(low)
    col_cos, col_sin = phase_pair(freq_ids, np.arange(cols, dtype=np.int32), cols)
    real_part = np.concatenate([col_cos.T, -col_sin.T], 1) / np.float32(cols)
    imag_part = np.concatenate([col_sin.T, col_cos.T], 1) / np.float32(cols)
    forward_cols = np.stack([real_part, imag_part], 0).astype(low)
    halves = []
    for part in range(SPLIT):
        at = slice(part * cols // SPLIT, (part + 1) * cols // SPLIT)
        halves.append(
            np.concatenate(
                [col_cos[:, at], -col_sin[:, at], col_sin[:, at], col_cos[:, at]],
                0,
            )
        )
    inverse_cols = np.concatenate(halves, 0).astype(low)
    inner_cos, inner_sin = phase_pair(freq_ids, np.arange(rows, dtype=np.int32) + HALO, win_len)
    inner_cos, inner_sin = (inner_cos.T, inner_sin.T)
    inverse_rows = np.stack(
        [np.stack([inner_cos, -inner_sin], 1), np.stack([inner_sin, inner_cos], 1)], 0
    ).astype(low)
    windows = np.stack(
        [
            inverse_rows[:, :, :, LOW + v * ALIGN : LOW + v * ALIGN + SPAN].reshape(2 * rows, 2 * SPAN)
            for v in range(VARIANTS)
        ],
        0,
    )
    inverse_rows_t = inverse_rows.transpose(2, 3, 0, 1).reshape(2 * FREQ, 2 * rows)
    back = np.concatenate([forward_rows[HALF:FREQ], forward_rows[FREQ + HALF :]], 0).T
    back = np.concatenate([back, back], 1)
    windows = np.pad(windows, ((0, 0), (0, 0), (0, win_len - 2 * SPAN)))
    late = np.concatenate([*windows, inverse_rows_t, back, inverse_cols], 0)
    return (forward_rows, forward_cols, late)


def dot(a, b):
    return jnp.dot(a, b, preferred_element_type=jnp.float32)


def dot_t(a, b):
    return lax.dot_general(a, b, (((1,), (1,)), ((), ())), preferred_element_type=jnp.float32)


def start_sources(packs, small_ref, sem):
    copies = [pltpu.make_async_copy(pack, small_ref.at[d], sem.at[d]) for d, pack in enumerate(packs)]
    for copy in copies:
        copy.start()
    return copies


def read_sources(copies, small_ref, at_ref, weight_ref):
    for copy in copies:
        copy.wait()
    per = at_ref.shape[1] // len(copies)
    for d in range(len(copies)):
        for i in range(per):
            s = d * per + i
            along_k = small_ref[d, 0, 3 * i].astype(jnp.int32)
            first = FREQ // 2 - RADIUS - along_k
            at_ref[0, s] = first - lax.rem(first, ALIGN)
            at_ref[1, s] = along_k - FREQ // 2
            at_ref[2, s] = small_ref[d, 0, 3 * i + 1].astype(jnp.int32) - FREQ // 2
            weight_ref[s] = small_ref[d, 0, 3 * i + 2]


def window_of(at_ref, s):
    return pl.multiple_of(at_ref[0, s], ALIGN)


def image(mask, unpack, shift_ref, weight_ref, tables, target_ref, partial_ref, resist_ref, scratch, rows):
    fr_ref, fc_ref, late_ref = tables
    per_window = 2 * rows
    first_t = VARIANTS * per_window
    at = first_t + 2 * per_window

    def col_table(q):
        return late_ref[at + 2 * q * FREQ : at + 2 * (q + 1) * FREQ, :]

    spec_ref, pupil_ref, cols_ref, field_ref, dcols_ref, inten_ref, acc_ref = scratch
    sources = field_ref.shape[0]
    width = field_ref.shape[2]
    half = dot(fr_ref[...], mask).astype(jnp.bfloat16)
    spectrum = dot(half[:FREQ], fc_ref[0]) + dot(half[FREQ:], fc_ref[1])
    spec_ref[...] = spectrum.astype(jnp.bfloat16).astype(jnp.float32)
    inten_ref[...] = jnp.zeros_like(inten_ref)
    acc_ref[...] = jnp.zeros_like(acc_ref)
    unpack()

    def to_columns(g):
        pieces = []
        for i in range(GROUP):
            s = g * GROUP + i
            base = window_of(shift_ref, s)
            along_k = lax.broadcasted_iota(jnp.int32, (SPAN, FREQ), 0) + (base + shift_ref[1, s])
            along_l = lax.broadcasted_iota(jnp.int32, (SPAN, FREQ), 1) + shift_ref[2, s]
            inside = along_k * along_k + along_l * along_l <= RADIUS * RADIUS
            pupil = jnp.where(inside, 1.0, 0.0)
            pupil_ref[s] = pupil
            part = spec_ref[pl.ds(base, SPAN), :]
            pieces.append((part * jnp.concatenate([pupil, pupil], 1)).astype(jnp.bfloat16))
        passed = jnp.concatenate(pieces, 0)
        for q in range(2):
            out = dot(passed, col_table(q)).astype(jnp.bfloat16)
            for i in range(GROUP):
                cols_ref[g * GROUP + i, q * SPAN : (q + 1) * SPAN, :] = out[i * SPAN : (i + 1) * SPAN]

    def to_field(g):
        total = inten_ref[...]
        for i in range(STEP):
            s = g * STEP + i
            variant = lax.div(shift_ref[0, s] - LOW, ALIGN)
            field = dot(late_ref[pl.ds(pl.multiple_of(variant * per_window, per_window), per_window), : 2 * SPAN], cols_ref[s])
            field_ref[s] = field
            scaled = weight_ref[s] * (1.0 / sources)
            total = total + scaled * (field[:rows] * field[:rows] + field[rows:] * field[rows:])
        inten_ref[...] = total

    groups, per = sources // GROUP, GROUP // STEP
    to_columns(0)
    for g in range(groups):
        if g + 1 < groups:
            to_columns(g + 1)
        for h in range(per):
            to_field(g * per + h)

    resist = jax.nn.sigmoid(steepness * (inten_ref[...] - dose_level))
    if resist_ref is not None:
        resist_ref[...] = resist
    goal = target_ref[...].astype(jnp.float32)
    inten_ref[...] = 2.0 * (resist - goal) * steepness * resist * (1.0 - resist)

    def to_d_columns(g):
        d_int = inten_ref[...]
        for i in range(STEP):
            s = g * STEP + i
            base = window_of(shift_ref, s)
            scale = d_int * (2.0 * weight_ref[s] * (1.0 / sources))
            d_field = (field_ref[s] * jnp.concatenate([scale, scale], 0)).astype(jnp.bfloat16)
            table = jnp.concatenate(
                [late_ref[pl.ds(pl.multiple_of(first_t + base + q * FREQ, ALIGN), SPAN), :] for q in range(2)], 0
            )
            d_cols = dot(table, d_field).astype(jnp.bfloat16)
            dcols_ref[s, :, :width] = d_cols[:SPAN]
            dcols_ref[s, :, width:] = d_cols[SPAN:]

    def to_d_spectrum(g):
        d_cols = dcols_ref[pl.ds(g * GROUP, GROUP)].reshape(GROUP * SPAN, 2 * width)
        d_passed = dot_t(d_cols[:, :width], col_table(0)) + dot_t(d_cols[:, width:], col_table(1))
        for i in range(GROUP):
            s = g * GROUP + i
            base = window_of(shift_ref, s)
            pupil = pupil_ref[s]
            part = d_passed[i * SPAN : (i + 1) * SPAN] * jnp.concatenate([pupil, pupil], 1)
            acc_ref[pl.ds(base, SPAN), :] = acc_ref[pl.ds(base, SPAN), :] + part

    for g in range(groups):
        for h in range(per):
            to_d_columns(g * per + h)
        if g > 0:
            to_d_spectrum(g - 1)
    to_d_spectrum(groups - 1)
    partial_ref[...] = folded(acc_ref)


def thirds(x):
    high = x.astype(jnp.bfloat16)
    left = x - high.astype(jnp.float32)
    mid = left.astype(jnp.bfloat16)
    return high, mid, (left - mid.astype(jnp.float32)).astype(jnp.bfloat16)


def folded(acc_ref):
    i = lax.broadcasted_iota(jnp.int32, (HALF, HALF), 0)
    j = lax.broadcasted_iota(jnp.int32, (HALF, HALF), 1)
    turn_k = jnp.where(i + j == HALF, 1.0, 0.0).astype(jnp.bfloat16)
    i = lax.broadcasted_iota(jnp.int32, (2 * FREQ, 2 * FREQ), 0)
    j = lax.broadcasted_iota(jnp.int32, (2 * FREQ, 2 * FREQ), 1)
    turn_l = jnp.where(i + j == FREQ, 1.0, 0.0) - jnp.where((i + j == 3 * FREQ) & (i >= FREQ) & (j >= FREQ), 1.0, 0.0)
    turn_l = jnp.where((i < FREQ) == (j < FREQ), turn_l, 0.0).astype(jnp.bfloat16)
    parts = jnp.concatenate(thirds(acc_ref[:HALF, :]), 1)
    turned = dot(turn_k, parts).astype(jnp.bfloat16)
    turned = jnp.concatenate([turned[:, p * 2 * FREQ : (p + 1) * 2 * FREQ] for p in range(3)], 0)
    turned = dot(turned, turn_l)
    turned = turned[:HALF] + turned[HALF : 2 * HALF] + turned[2 * HALF :]
    return acc_ref[HALF : HALF + FOLD, :] + turned[:FOLD]


def d_halves(sums, half, fc_ref, dsum_ref, dhalf_ref, count):
    exact = sums[0].dtype == jnp.bfloat16
    zero = jnp.zeros((HALF - FOLD, 2 * FREQ), jnp.float32)

    def one(o, total):
        total = jnp.concatenate([total.astype(jnp.float32), zero], 0)
        high = total.astype(jnp.bfloat16)
        at = pl.multiple_of(o * HALF, HALF)
        dsum_ref[pl.ds(at, HALF), :] = high
        if not exact:
            rest = (total - high.astype(jnp.float32)).astype(jnp.bfloat16)
            dsum_ref[pl.ds(pl.multiple_of(at + count * HALF, HALF), HALF), :] = rest

    one(0, sums[0][...])
    for (low, high), mine, other in zip(pairs_of(count), sums[1::2], sums[2::2]):
        if low == high:
            first = jnp.where(half == 0, mine[...], other[...])
            second = jnp.where(half == 0, other[...], mine[...])
            one(low, jnp.concatenate([first, second], 1))
        else:
            one(jnp.where(half == 0, low, high), mine[...])
            one(jnp.where(half == 0, high, low), other[...])
    span = count * HALF
    d_sum = dsum_ref[:span, :] if exact else dsum_ref[...]
    for p in range(2):
        d_half = dot_t(d_sum, fc_ref[p])
        if not exact:
            d_half = d_half[:span] + d_half[span:]
        d_high = d_half.astype(jnp.bfloat16)
        d_rest = (d_half - d_high.astype(jnp.float32)).astype(jnp.bfloat16)
        for o in range(count):
            dhalf_ref[o, p * HALF : (p + 1) * HALF, :] = d_high[o * HALF : (o + 1) * HALF]
            dhalf_ref[o, FREQ + p * HALF : FREQ + (p + 1) * HALF, :] = d_rest[o * HALF : (o + 1) * HALF]


def put_block(field_ref, i, rows, value):
    width = field_ref.shape[2]
    for h in range(SPLIT):
        field_ref[SPLIT * i + h, :rows, :] = value[:, h * width : (h + 1) * width]


def get_block(field_ref, i, rows):
    return jnp.concatenate([field_ref[SPLIT * i + h, :rows, :] for h in range(SPLIT)], 1)


def gradients(blocks, late_ref, dhalf_ref, field_ref, rows, cols):
    count = len(blocks)
    at = late_ref.shape[0] - 4 * FREQ - 2 * rows
    squares = jnp.zeros((1, 1), jnp.float32)
    for i, block in enumerate(blocks):
        m = jax.nn.sigmoid(block())
        d_mask = dot(late_ref[at : at + rows, :], dhalf_ref[i]) + dot(late_ref[at + rows : at + 2 * rows, :], dhalf_ref[(i - 1) % count])
        d_theta = d_mask * m * (1.0 - m)
        put_block(field_ref, i, rows, d_theta)
        squares = squares + jnp.sum(d_theta * d_theta, axis=(0, 1), keepdims=True)
    return step_size * lax.rsqrt(squares / (rows * count * cols) + epsilon)


def blocks_of(state_refs, half, count, rows):
    def at(ref, row):
        return lambda: ref[row : row + HALO, :].astype(jnp.float32)

    def exact(ref):
        return lambda: ref[:HALO, :].astype(jnp.float32) + ref[HALO : 2 * HALO, :].astype(jnp.float32)

    def pick(even, odd):
        return lambda: jnp.where(half == 0, even(), odd())

    if half is None:
        pieces = [at(ref, row) for ref in state_refs for row in range(0, ref.shape[0], HALO)]
    else:
        own, mine, other = state_refs[:3]
        pieces = [pick(exact(mine), exact(other)), at(own, 0), at(own, HALO), pick(exact(other), exact(mine))]
        pieces += [pick(at(other, 2 * HALO), at(mine, 2 * HALO))]
        for far_mine, far_other in zip(state_refs[3::2], state_refs[4::2]):
            pieces += [pick(at(far_mine, 0), at(far_other, 0)), pick(at(far_other, 0), at(far_mine, 0))]
        pieces += [pick(at(mine, 2 * HALO), at(other, 2 * HALO))]
    per = rows // HALO

    def load(i):
        return jnp.concatenate([piece() for piece in pieces[i * per : (i + 1) * per]], 0)

    return [functools.partial(load, i) for i in range(count)]


def prepare_kernel(half_ref, shift_in, weight_in, theta_ref, fr_ref, fc_ref, late_in, target_in, fr_out, fc_out, late_out, target_out, own_out, halo_out, near_out, far_out, pack_out, shift_ref, weight_ref, sems):
    half = half_ref[0]
    theta_copy = pltpu.make_async_copy(theta_ref, own_out, sems.at[2])
    theta_copy.start()
    points = [pltpu.make_async_copy(shift_in, shift_ref, sems.at[3]), pltpu.make_async_copy(weight_in, weight_ref, sems.at[4])]
    width = target_out.shape[1]
    column = pl.multiple_of(half * width, width)
    tail = 4 * FREQ
    split = late_out.shape[0] - tail
    mine = pl.multiple_of(split + half * tail, tail // 2)
    copies = [
        (fr_ref, fr_out),
        (fc_ref, fc_out),
        (late_in.at[:split, :], late_out.at[:split, :]),
        (late_in.at[pl.ds(mine, tail), :], late_out.at[split:, :]),
        (target_in.at[:, pl.ds(column, width)], target_out),
    ]
    copies = [pltpu.make_async_copy(a, b, sems.at[5 + i]) for i, (a, b) in enumerate(copies)]
    for copy in points + copies:
        copy.start()
    for copy in points:
        copy.wait()
    row = lax.broadcasted_iota(jnp.int32, pack_out.shape, 0)
    lane = lax.broadcasted_iota(jnp.int32, pack_out.shape, 1)
    pack = jnp.zeros(pack_out.shape, jnp.float32)
    for i in range(weight_ref.shape[0]):
        for j, value in enumerate(
            (shift_ref[0, i].astype(jnp.float32), shift_ref[1, i].astype(jnp.float32), weight_ref[i])
        ):
            pack = jnp.where((row == 0) & (lane == 3 * i + j), value, pack)
    pack_out[...] = pack
    theta_copy.wait()
    rows = own_out.shape[0]
    even = half == 0
    head, tail = own_out[:HALO, :], own_out[rows - HALO :, :]
    toward, away = jnp.where(even, tail, head), jnp.where(even, head, tail)
    halo_out[...] = jax.nn.sigmoid(toward).astype(jnp.bfloat16)
    high = toward.astype(jnp.bfloat16)
    near_out[:HALO, :] = high
    near_out[HALO : 2 * HALO, :] = (toward - high.astype(jnp.float32)).astype(jnp.bfloat16)
    near_out[2 * HALO :, :] = away.astype(jnp.bfloat16)
    far_out[...] = away.astype(jnp.bfloat16)
    for copy in copies:
        copy.wait()


def first_kernel(n_packs, *refs):
    half_ref, packs, refs = refs[0], refs[1 : 1 + n_packs], refs[1 + n_packs :]
    mine_ref, other_ref, own_ref, fr_ref, fc_ref, late_ref, target_ref, partial_ref = refs[:8]
    at_ref, weight_ref, small_ref, sem = refs[8:12]
    scratch = refs[12:]
    half = half_ref[0]
    rows = own_ref.shape[0]
    copies = start_sources(packs, small_ref, sem)
    unpack = functools.partial(read_sources, copies, small_ref, at_ref, weight_ref)
    first = half == 0
    mine, other = mine_ref[...].astype(jnp.float32), other_ref[...].astype(jnp.float32)
    own = jax.nn.sigmoid(own_ref[...]).astype(jnp.bfloat16)
    before = jnp.where(first, mine, other).astype(jnp.bfloat16)
    after = jnp.where(first, other, mine).astype(jnp.bfloat16)
    mask = jnp.concatenate([before, own, after], 0)
    image(mask, unpack, at_ref, weight_ref, (fr_ref, fc_ref, late_ref), target_ref, partial_ref, None, scratch, rows)


def later_kernel(count, n_packs, n_sums, n_state, gathered, *refs):
    half_ref, packs, refs = refs[0], refs[1 : 1 + n_packs], refs[1 + n_packs :]
    sums, state, refs = refs[:n_sums], refs[n_sums : n_sums + n_state], refs[n_sums + n_state :]
    fr_ref, fc_ref, late_ref, target_ref = refs[:4]
    partial_ref, resist_ref, window_out, rest_out = refs[4:8]
    at_ref, weight_ref, small_ref, sem = refs[8:12]
    scratch, (dsum_ref, dhalf_ref) = refs[12:19], refs[19:]
    field_ref = scratch[3]
    rows, cols = window_out.shape[0] // 2, window_out.shape[1]
    half = half_ref[0]
    copies = start_sources(packs, small_ref, sem)
    unpack = functools.partial(read_sources, copies, small_ref, at_ref, weight_ref)
    blocks = blocks_of(state, None if gathered else half, count, rows)
    d_halves(sums, half, fc_ref, dsum_ref, dhalf_ref, count)
    factor = gradients(blocks, late_ref, dhalf_ref, field_ref, rows, cols)
    masks = []
    for i, block in enumerate(blocks):
        theta = block() - get_block(field_ref, i, rows) * factor
        if i < 2:
            window_out[i * rows : (i + 1) * rows, :] = theta
            masks.append(jax.nn.sigmoid(theta).astype(jnp.bfloat16))
        else:
            rest_out[(i - 2) * rows : (i - 1) * rows, :] = theta
    image(jnp.concatenate(masks, 0), unpack, at_ref, weight_ref, (fr_ref, fc_ref, late_ref), target_ref, partial_ref, resist_ref, scratch, rows)


def last_kernel(count, n_sums, *refs):
    half_ref, refs = refs[0], refs[1:]
    sums, state, refs = refs[:n_sums], refs[n_sums : n_sums + 2], refs[n_sums + 2 :]
    fc_ref, late_ref, resist_ref, resist_other, theta_out, resist_out, field_ref, dsum_ref, dhalf_ref = refs
    rows, cols = theta_out.shape
    width = resist_ref.shape[1]
    half = half_ref[0]
    d_halves(sums, half, fc_ref, dsum_ref, dhalf_ref, count)
    factor = gradients(blocks_of(state, None, count, rows), late_ref, dhalf_ref, field_ref, rows, cols)
    d_own = jnp.concatenate([get_block(field_ref, 0, rows)[HALO:], get_block(field_ref, 1, rows)[: rows - HALO]], 0)
    theta_out[...] = state[0][HALO : HALO + rows, :] - d_own * factor
    first = half == 0
    resist_out[:, :width] = jnp.where(first, resist_ref[...], resist_other[...])
    resist_out[:, width:] = jnp.where(first, resist_other[...], resist_ref[...])


def pairs_of(count):
    return [(o, count - o) for o in range(1, (count + 1) // 2)] + [(count // 2, count // 2)] * (count % 2 == 0)


def fetch(array, low, high, across=0):
    strips, size = lax.axis_size("strip"), lax.axis_size("src")
    steps = [
        ((z + (high if s % SPLIT else low)) % strips * size + (s + SPLIT * across) % size, z * size + s)
        for z in range(strips)
        for s in range(size)
    ]
    return lax.ppermute(array, ("strip", "src"), steps)


def exchange(partial, half, dtype):
    total = (partial + partner(partial)).astype(dtype)
    sums = [total]
    for low, high in pairs_of(lax.axis_size("strip")):
        send = total
        if low == high:
            send = jnp.where(half == 0, total[:, :FREQ], total[:, FREQ:])
        mine = fetch(send, low, high)
        sums += [mine, partner(mine)]
    return sums


def per_device_body(theta, target, source_shift, source_weight):
    rows, cols = theta.shape
    count = lax.axis_size("strip")
    n_src = lax.axis_size("src")
    width = cols // SPLIT
    sources = source_weight.shape[0] * n_src
    half = (lax.axis_index("src") % SPLIT).astype(jnp.int32)
    forward_rows, forward_cols, late = [jnp.asarray(t) for t in build_tables(rows, cols)]
    vmem = pl.BlockSpec(memory_space=pltpu.VMEM)
    smem = pl.BlockSpec(memory_space=pltpu.SMEM)
    f32 = jnp.float32

    far_space = pl.BlockSpec(memory_space=pltpu.HBM)
    low = jnp.bfloat16
    outs = [pltpu.VMEM(a.shape, a.dtype) for a in (forward_rows, forward_cols)]
    outs += [pltpu.VMEM((late.shape[0] - (SPLIT - 1) * 4 * FREQ, late.shape[1]), late.dtype)]
    outs += [pltpu.VMEM((rows, width), jnp.int32), pltpu.VMEM(theta.shape, f32)]
    outs += [pltpu.VMEM((HALO, cols), low), pltpu.VMEM((3 * HALO, cols), low), pltpu.VMEM((HALO, cols), low)]
    outs += [pltpu.VMEM((8, FREQ), f32)]
    forward_rows, forward_cols, late, target, theta, halo, near, far, pack = pl.pallas_call(
        prepare_kernel,
        out_shape=outs,
        in_specs=[smem] + [far_space] * 7,
        out_specs=[vmem] * len(outs),
        scratch_shapes=[
            pltpu.SMEM(source_shift.shape[::-1], jnp.int32),
            pltpu.SMEM(source_weight.shape, f32),
            pltpu.SemaphoreType.DMA((10,)),
        ],
        name="prepare",
    )(half.reshape(1), source_shift.T, source_weight, theta, forward_rows, forward_cols, late, target)
    mine = fetch(halo, count - 1, 1)
    packs = [pack] + [shifted(pack, "src", SPLIT * k) for k in range(1, n_src // SPLIT)]
    packs = [a for one in packs for a in (one, partner(one))]
    halo = [mine, partner(mine)]
    fetched = [fetch(near, count - 1, 1)] + [fetch(far, o, o) for o in range(2, count - 1)]
    pieces = [a for mine in fetched for a in (mine, partner(mine))]

    source_scratch = [
        pltpu.SMEM((3, sources), jnp.int32),
        pltpu.SMEM((sources,), f32),
        pltpu.SMEM((n_src, 8, FREQ), f32),
        pltpu.SemaphoreType.DMA((n_src,)),
    ]
    image_scratch = [
        pltpu.VMEM((FREQ, 2 * FREQ), f32),
        pltpu.VMEM((sources, SPAN, FREQ), f32),
        pltpu.VMEM((sources, 2 * SPAN, width), jnp.bfloat16),
        pltpu.VMEM((sources, 2 * rows, width), f32),
        pltpu.VMEM((sources, SPAN, 2 * width), jnp.bfloat16),
        pltpu.VMEM((rows, width), f32),
        pltpu.VMEM((FREQ, 2 * FREQ), f32),
    ]
    adjoint_scratch = [
        pltpu.VMEM((2 * count * HALF, 2 * FREQ), jnp.bfloat16),
        pltpu.VMEM((count, 2 * FREQ, cols), jnp.bfloat16),
    ]

    def call(kernel, args, outs, scratch, flops):
        outs = [jax.ShapeDtypeStruct(shape, dtype) for shape, dtype in outs]
        arrays = [*args, *outs, *[a for a in scratch if a.dtype in (f32, jnp.bfloat16)]]
        held = sum(math.prod(a.shape) * jnp.dtype(a.dtype).itemsize for a in arrays)
        return pl.pallas_call(
            kernel,
            out_shape=outs,
            in_specs=[smem] + [vmem] * (len(args) - 1),
            out_specs=[vmem] * len(outs),
            scratch_shapes=scratch,
            compiler_params=pltpu.CompilerParams(vmem_limit_bytes=held + (6 << 20)),
            cost_estimate=pl.CostEstimate(flops=flops, bytes_accessed=4 << 20, transcendentals=1 << 20),
        )(*args)

    smalls = [half.reshape(1), *packs]
    n_packs = len(packs)
    partial_shape = ((FOLD, 2 * FREQ), f32)
    (partial,) = call(
        functools.partial(first_kernel, n_packs),
        [*smalls, *halo, theta, forward_rows, forward_cols, late, target],
        [partial_shape],
        source_scratch + image_scratch,
        6 << 30,
    )
    state, gathered = [theta, *pieces], False
    for _ in range(ITERS - 1):
        sums = exchange(partial, half, f32)
        partial, resist, *state = call(
            functools.partial(later_kernel, count, n_packs, len(sums), len(state), gathered),
            [*smalls, *sums, *state, forward_rows, forward_cols, late, target],
            [partial_shape, ((rows, width), f32), ((2 * rows, cols), f32), (((count - 2) * rows, cols), f32)],
            source_scratch + image_scratch + adjoint_scratch,
            6 << 30,
        )
        gathered = True
    sums = exchange(partial, half, jnp.bfloat16)
    theta, resist = call(
        functools.partial(last_kernel, count, len(sums)),
        [half.reshape(1), *sums, *state, forward_cols, late, resist, partner(resist)],
        [((rows, cols), f32)] * 2,
        [pltpu.VMEM((SPLIT * count, rows, width), f32)] + adjoint_scratch,
        1 << 30,
    )
    return (theta, resist)


def solution(mesh):
    return jax.shard_map(
        per_device_body,
        mesh=mesh,
        in_specs=(P(("band", "strip"), None), P(("band", "strip"), None), P("src", None), P("src")),
        out_specs=(P(("band", "strip"), None), P(("band", "strip"), None)),
        check_vma=False,
    )
```

```python
import functools
import math

import jax
import jax.numpy as jnp
import numpy as np
from jax import lax
from jax.experimental import pallas as pl
from jax.experimental.pallas import tpu as pltpu
from jax.sharding import PartitionSpec as P


HALO = 64
FREQ = 128
ITERS = 2

steepness = 20.0
dose_level = 0.27
step_size = 1.0
epsilon = 1e-06

RADIUS = FREQ // 4
MAX_SHIFT = FREQ // 8
LOW = FREQ // 2 - RADIUS - MAX_SHIFT
FOLD = -(-(RADIUS + MAX_SHIFT + 1) // 8) * 8
HALF = FREQ // 2
ALIGN = 16
SPAN = 2 * RADIUS + ALIGN
VARIANTS = 2 * MAX_SHIFT // ALIGN + 1
SPLIT = 2
GROUP = 4
STEP = 4


def shifted(array, axis, by):
    size = lax.axis_size(axis)
    return lax.ppermute(array, axis, [(i, (i + by) % size) for i in range(size)])


def partner(array):
    size = lax.axis_size("src")
    return lax.ppermute(array, "src", [(i, i ^ 1) for i in range(size)])


def phase_pair(freq_ids, points, period):
    index = freq_ids[:, None] % period * points[None, :] % period
    angle = np.float32(2.0 * math.pi / period) * index.astype(np.float32)
    return (np.cos(angle), np.sin(angle))


@functools.lru_cache(maxsize=None)
def build_tables(rows, cols):
    low = jnp.bfloat16
    freq_ids = np.arange(FREQ, dtype=np.int32) - FREQ // 2
    win_len = rows + 2 * HALO
    row_cos, row_sin = phase_pair(freq_ids, np.arange(win_len, dtype=np.int32), win_len)
    forward_rows = (np.concatenate([row_cos, -row_sin], 0) / np.float32(win_len)).astype(low)
    col_cos, col_sin = phase_pair(freq_ids, np.arange(cols, dtype=np.int32), cols)
    real_part = np.concatenate([col_cos.T, -col_sin.T], 1) / np.float32(cols)
    imag_part = np.concatenate([col_sin.T, col_cos.T], 1) / np.float32(cols)
    forward_cols = np.stack([real_part, imag_part], 0).astype(low)
    halves = []
    for part in range(SPLIT):
        at = slice(part * cols // SPLIT, (part + 1) * cols // SPLIT)
        halves.append(
            np.concatenate(
                [col_cos[:, at], -col_sin[:, at], col_sin[:, at], col_cos[:, at]],
                0,
            )
        )
    inverse_cols = np.concatenate(halves, 0).astype(low)
    inner_cos, inner_sin = phase_pair(freq_ids, np.arange(rows, dtype=np.int32) + HALO, win_len)
    inner_cos, inner_sin = (inner_cos.T, inner_sin.T)
    inverse_rows = np.stack(
        [np.stack([inner_cos, -inner_sin], 1), np.stack([inner_sin, inner_cos], 1)], 0
    ).astype(low)
    windows = np.stack(
        [
            inverse_rows[:, :, :, LOW + v * ALIGN : LOW + v * ALIGN + SPAN].reshape(2 * rows, 2 * SPAN)
            for v in range(VARIANTS)
        ],
        0,
    )
    inverse_rows_t = inverse_rows.transpose(2, 3, 0, 1).reshape(2 * FREQ, 2 * rows)
    back = np.concatenate([forward_rows[HALF:FREQ], forward_rows[FREQ + HALF :]], 0).T
    back = np.concatenate([back, back], 1)
    windows = np.pad(windows, ((0, 0), (0, 0), (0, win_len - 2 * SPAN)))
    late = np.concatenate([*windows, inverse_rows_t, back, inverse_cols], 0)
    return (forward_rows, forward_cols, late)


def dot(a, b):
    return jnp.dot(a, b, preferred_element_type=jnp.float32)


def dot_t(a, b):
    return lax.dot_general(a, b, (((1,), (1,)), ((), ())), preferred_element_type=jnp.float32)


def start_sources(packs, small_ref, sem):
    copies = [pltpu.make_async_copy(pack, small_ref.at[d], sem.at[d]) for d, pack in enumerate(packs)]
    for copy in copies:
        copy.start()
    return copies


def read_sources(copies, small_ref, at_ref, weight_ref):
    for copy in copies:
        copy.wait()
    per = at_ref.shape[1] // len(copies)
    for d in range(len(copies)):
        for i in range(per):
            s = d * per + i
            along_k = small_ref[d, 0, 3 * i].astype(jnp.int32)
            first = FREQ // 2 - RADIUS - along_k
            at_ref[0, s] = first - lax.rem(first, ALIGN)
            at_ref[1, s] = along_k - FREQ // 2
            at_ref[2, s] = small_ref[d, 0, 3 * i + 1].astype(jnp.int32) - FREQ // 2
            weight_ref[s] = small_ref[d, 0, 3 * i + 2]


def window_of(at_ref, s):
    return pl.multiple_of(at_ref[0, s], ALIGN)


def image(mask, unpack, shift_ref, weight_ref, tables, target_ref, partial_ref, resist_ref, scratch, rows):
    fr_ref, fc_ref, late_ref = tables
    per_window = 2 * rows
    first_t = VARIANTS * per_window
    at = first_t + 2 * per_window

    def col_table(q):
        return late_ref[at + 2 * q * FREQ : at + 2 * (q + 1) * FREQ, :]

    spec_ref, pupil_ref, cols_ref, field_ref, dcols_ref, inten_ref, acc_ref = scratch
    sources = field_ref.shape[0]
    width = field_ref.shape[2]
    half = dot(fr_ref[...], mask).astype(jnp.bfloat16)
    spectrum = dot(half[:FREQ], fc_ref[0]) + dot(half[FREQ:], fc_ref[1])
    spec_ref[...] = spectrum.astype(jnp.bfloat16).astype(jnp.float32)
    inten_ref[...] = jnp.zeros_like(inten_ref)
    acc_ref[...] = jnp.zeros_like(acc_ref)
    unpack()

    def to_columns(g):
        pieces = []
        for i in range(GROUP):
            s = g * GROUP + i
            base = window_of(shift_ref, s)
            along_k = lax.broadcasted_iota(jnp.int32, (SPAN, FREQ), 0) + (base + shift_ref[1, s])
            along_l = lax.broadcasted_iota(jnp.int32, (SPAN, FREQ), 1) + shift_ref[2, s]
            inside = along_k * along_k + along_l * along_l <= RADIUS * RADIUS
            pupil = jnp.where(inside, 1.0, 0.0)
            pupil_ref[s] = pupil
            part = spec_ref[pl.ds(base, SPAN), :]
            pieces.append((part * jnp.concatenate([pupil, pupil], 1)).astype(jnp.bfloat16))
        passed = jnp.concatenate(pieces, 0)
        for q in range(2):
            out = dot(passed, col_table(q)).astype(jnp.bfloat16)
            for i in range(GROUP):
                cols_ref[g * GROUP + i, q * SPAN : (q + 1) * SPAN, :] = out[i * SPAN : (i + 1) * SPAN]

    def to_field(g):
        total = inten_ref[...]
        for i in range(STEP):
            s = g * STEP + i
            variant = lax.div(shift_ref[0, s] - LOW, ALIGN)
            field = dot(late_ref[pl.ds(pl.multiple_of(variant * per_window, per_window), per_window), : 2 * SPAN], cols_ref[s])
            field_ref[s] = field
            scaled = weight_ref[s] * (1.0 / sources)
            total = total + scaled * (field[:rows] * field[:rows] + field[rows:] * field[rows:])
        inten_ref[...] = total

    groups, per = sources // GROUP, GROUP // STEP
    to_columns(0)
    for g in range(groups):
        if g + 1 < groups:
            to_columns(g + 1)
        for h in range(per):
            to_field(g * per + h)

    resist = jax.nn.sigmoid(steepness * (inten_ref[...] - dose_level))
    if resist_ref is not None:
        resist_ref[...] = resist
    goal = target_ref[...].astype(jnp.float32)
    inten_ref[...] = 2.0 * (resist - goal) * steepness * resist * (1.0 - resist)

    def to_d_columns(g):
        d_int = inten_ref[...]
        for i in range(STEP):
            s = g * STEP + i
            base = window_of(shift_ref, s)
            scale = d_int * (2.0 * weight_ref[s] * (1.0 / sources))
            d_field = (field_ref[s] * jnp.concatenate([scale, scale], 0)).astype(jnp.bfloat16)
            table = jnp.concatenate(
                [late_ref[pl.ds(pl.multiple_of(first_t + base + q * FREQ, ALIGN), SPAN), :] for q in range(2)], 0
            )
            d_cols = dot(table, d_field).astype(jnp.bfloat16)
            dcols_ref[s, :, :width] = d_cols[:SPAN]
            dcols_ref[s, :, width:] = d_cols[SPAN:]

    def to_d_spectrum(g):
        d_cols = dcols_ref[pl.ds(g * GROUP, GROUP)].reshape(GROUP * SPAN, 2 * width)
        d_passed = dot_t(d_cols[:, :width], col_table(0)) + dot_t(d_cols[:, width:], col_table(1))
        for i in range(GROUP):
            s = g * GROUP + i
            base = window_of(shift_ref, s)
            pupil = pupil_ref[s]
            part = d_passed[i * SPAN : (i + 1) * SPAN] * jnp.concatenate([pupil, pupil], 1)
            acc_ref[pl.ds(base, SPAN), :] = acc_ref[pl.ds(base, SPAN), :] + part

    @pl.when(shift_ref[0, 0] >= 0)
    def _():
        for g in range(groups):
            for h in range(per):
                to_d_columns(g * per + h)
            if g > 0:
                to_d_spectrum(g - 1)
        to_d_spectrum(groups - 1)
        partial_ref[...] = folded(acc_ref)


def thirds(x):
    high = x.astype(jnp.bfloat16)
    left = x - high.astype(jnp.float32)
    mid = left.astype(jnp.bfloat16)
    return high, mid, (left - mid.astype(jnp.float32)).astype(jnp.bfloat16)


def folded(acc_ref):
    i = lax.broadcasted_iota(jnp.int32, (HALF, HALF), 0)
    j = lax.broadcasted_iota(jnp.int32, (HALF, HALF), 1)
    turn_k = jnp.where(i + j == HALF, 1.0, 0.0).astype(jnp.bfloat16)
    i = lax.broadcasted_iota(jnp.int32, (2 * FREQ, 2 * FREQ), 0)
    j = lax.broadcasted_iota(jnp.int32, (2 * FREQ, 2 * FREQ), 1)
    turn_l = jnp.where(i + j == FREQ, 1.0, 0.0) - jnp.where((i + j == 3 * FREQ) & (i >= FREQ) & (j >= FREQ), 1.0, 0.0)
    turn_l = jnp.where((i < FREQ) == (j < FREQ), turn_l, 0.0).astype(jnp.bfloat16)
    parts = jnp.concatenate(thirds(acc_ref[:HALF, :]), 1)
    turned = dot(turn_k, parts).astype(jnp.bfloat16)
    turned = jnp.concatenate([turned[:, p * 2 * FREQ : (p + 1) * 2 * FREQ] for p in range(3)], 0)
    turned = dot(turned, turn_l)
    turned = turned[:HALF] + turned[HALF : 2 * HALF] + turned[2 * HALF :]
    return acc_ref[HALF : HALF + FOLD, :] + turned[:FOLD]


def d_halves(sums, half, fc_ref, dsum_ref, dhalf_ref, count):
    exact = sums[0].dtype == jnp.bfloat16
    zero = jnp.zeros((HALF - FOLD, 2 * FREQ), jnp.float32)

    def one(o, total):
        total = jnp.concatenate([total.astype(jnp.float32), zero], 0)
        high = total.astype(jnp.bfloat16)
        at = pl.multiple_of(o * HALF, HALF)
        dsum_ref[pl.ds(at, HALF), :] = high
        if not exact:
            rest = (total - high.astype(jnp.float32)).astype(jnp.bfloat16)
            dsum_ref[pl.ds(pl.multiple_of(at + count * HALF, HALF), HALF), :] = rest

    one(0, sums[0][...])
    for (low, high), mine, other in zip(pairs_of(count), sums[1::2], sums[2::2]):
        if low == high:
            first = jnp.where(half == 0, mine[...], other[...])
            second = jnp.where(half == 0, other[...], mine[...])
            one(low, jnp.concatenate([first, second], 1))
        else:
            one(jnp.where(half == 0, low, high), mine[...])
            one(jnp.where(half == 0, high, low), other[...])
    span = count * HALF
    d_sum = dsum_ref[:span, :] if exact else dsum_ref[...]
    for p in range(2):
        d_half = dot_t(d_sum, fc_ref[p])
        if not exact:
            d_half = d_half[:span] + d_half[span:]
        d_high = d_half.astype(jnp.bfloat16)
        d_rest = (d_half - d_high.astype(jnp.float32)).astype(jnp.bfloat16)
        for o in range(count):
            dhalf_ref[o, p * HALF : (p + 1) * HALF, :] = d_high[o * HALF : (o + 1) * HALF]
            dhalf_ref[o, FREQ + p * HALF : FREQ + (p + 1) * HALF, :] = d_rest[o * HALF : (o + 1) * HALF]


def put_block(field_ref, i, rows, value):
    width = field_ref.shape[2]
    for h in range(SPLIT):
        field_ref[SPLIT * i + h, :rows, :] = value[:, h * width : (h + 1) * width]


def get_block(field_ref, i, rows):
    return jnp.concatenate([field_ref[SPLIT * i + h, :rows, :] for h in range(SPLIT)], 1)


def gradients(blocks, late_ref, dhalf_ref, field_ref, rows, cols):
    count = len(blocks)
    at = late_ref.shape[0] - 4 * FREQ - 2 * rows
    squares = jnp.zeros((1, 1), jnp.float32)
    for i, block in enumerate(blocks):
        m = jax.nn.sigmoid(block())
        d_mask = dot(late_ref[at : at + rows, :], dhalf_ref[i]) + dot(late_ref[at + rows : at + 2 * rows, :], dhalf_ref[(i - 1) % count])
        d_theta = d_mask * m * (1.0 - m)
        put_block(field_ref, i, rows, d_theta)
        squares = squares + jnp.sum(d_theta * d_theta, axis=(0, 1), keepdims=True)
    return step_size * lax.rsqrt(squares / (rows * count * cols) + epsilon)


def blocks_of(state_refs, half, count, rows):
    def at(ref, row):
        return lambda: ref[row : row + HALO, :].astype(jnp.float32)

    def exact(ref):
        return lambda: ref[:HALO, :].astype(jnp.float32) + ref[HALO : 2 * HALO, :].astype(jnp.float32)

    def pick(even, odd):
        return lambda: jnp.where(half == 0, even(), odd())

    if half is None:
        pieces = [at(ref, row) for ref in state_refs for row in range(0, ref.shape[0], HALO)]
    else:
        own, mine, other = state_refs[:3]
        pieces = [pick(exact(mine), exact(other)), at(own, 0), at(own, HALO), pick(exact(other), exact(mine))]
        pieces += [pick(at(other, 2 * HALO), at(mine, 2 * HALO))]
        for far_mine, far_other in zip(state_refs[3::2], state_refs[4::2]):
            pieces += [pick(at(far_mine, 0), at(far_other, 0)), pick(at(far_other, 0), at(far_mine, 0))]
        pieces += [pick(at(mine, 2 * HALO), at(other, 2 * HALO))]
    per = rows // HALO

    def load(i):
        return jnp.concatenate([piece() for piece in pieces[i * per : (i + 1) * per]], 0)

    return [functools.partial(load, i) for i in range(count)]


def prepare_kernel(half_ref, shift_in, weight_in, theta_ref, fr_ref, fc_ref, late_in, target_in, fr_out, fc_out, late_out, target_out, own_out, halo_out, near_out, far_out, pack_out, shift_ref, weight_ref, sems):
    half = half_ref[0]
    theta_copy = pltpu.make_async_copy(theta_ref, own_out, sems.at[2])
    theta_copy.start()
    points = [pltpu.make_async_copy(shift_in, shift_ref, sems.at[3]), pltpu.make_async_copy(weight_in, weight_ref, sems.at[4])]
    width = target_out.shape[1]
    column = pl.multiple_of(half * width, width)
    tail = 4 * FREQ
    split = late_out.shape[0] - tail
    mine = pl.multiple_of(split + half * tail, tail // 2)
    copies = [
        (fr_ref, fr_out),
        (fc_ref, fc_out),
        (late_in.at[:split, :], late_out.at[:split, :]),
        (late_in.at[pl.ds(mine, tail), :], late_out.at[split:, :]),
        (target_in.at[:, pl.ds(column, width)], target_out),
    ]
    copies = [pltpu.make_async_copy(a, b, sems.at[5 + i]) for i, (a, b) in enumerate(copies)]
    for copy in points + copies:
        copy.start()
    for copy in points:
        copy.wait()
    row = lax.broadcasted_iota(jnp.int32, pack_out.shape, 0)
    lane = lax.broadcasted_iota(jnp.int32, pack_out.shape, 1)
    pack = jnp.zeros(pack_out.shape, jnp.float32)
    for i in range(weight_ref.shape[0]):
        for j, value in enumerate(
            (shift_ref[0, i].astype(jnp.float32), shift_ref[1, i].astype(jnp.float32), weight_ref[i])
        ):
            pack = jnp.where((row == 0) & (lane == 3 * i + j), value, pack)
    pack_out[...] = pack
    theta_copy.wait()
    rows = own_out.shape[0]
    even = half == 0
    head, tail = own_out[:HALO, :], own_out[rows - HALO :, :]
    toward, away = jnp.where(even, tail, head), jnp.where(even, head, tail)
    halo_out[...] = jax.nn.sigmoid(toward).astype(jnp.bfloat16)
    high = toward.astype(jnp.bfloat16)
    near_out[:HALO, :] = high
    near_out[HALO : 2 * HALO, :] = (toward - high.astype(jnp.float32)).astype(jnp.bfloat16)
    near_out[2 * HALO :, :] = away.astype(jnp.bfloat16)
    far_out[...] = away.astype(jnp.bfloat16)
    for copy in copies:
        copy.wait()


def first_kernel(n_packs, *refs):
    half_ref, packs, refs = refs[0], refs[1 : 1 + n_packs], refs[1 + n_packs :]
    mine_ref, other_ref, own_ref, fr_ref, fc_ref, late_ref, target_ref, partial_ref = refs[:8]
    at_ref, weight_ref, small_ref, sem = refs[8:12]
    scratch = refs[12:]
    half = half_ref[0]
    rows = own_ref.shape[0]
    copies = start_sources(packs, small_ref, sem)
    unpack = functools.partial(read_sources, copies, small_ref, at_ref, weight_ref)
    first = half == 0
    mine, other = mine_ref[...].astype(jnp.float32), other_ref[...].astype(jnp.float32)
    own = jax.nn.sigmoid(own_ref[...]).astype(jnp.bfloat16)
    before = jnp.where(first, mine, other).astype(jnp.bfloat16)
    after = jnp.where(first, other, mine).astype(jnp.bfloat16)
    mask = jnp.concatenate([before, own, after], 0)
    image(mask, unpack, at_ref, weight_ref, (fr_ref, fc_ref, late_ref), target_ref, partial_ref, None, scratch, rows)


def later_kernel(count, n_packs, n_sums, n_state, gathered, *refs):
    half_ref, packs, refs = refs[0], refs[1 : 1 + n_packs], refs[1 + n_packs :]
    sums, state, refs = refs[:n_sums], refs[n_sums : n_sums + n_state], refs[n_sums + n_state :]
    fr_ref, fc_ref, late_ref, target_ref = refs[:4]
    partial_ref, resist_ref, window_out, rest_out = refs[4:8]
    at_ref, weight_ref, small_ref, sem = refs[8:12]
    scratch, (dsum_ref, dhalf_ref) = refs[12:19], refs[19:]
    field_ref = scratch[3]
    rows, cols = window_out.shape[0] // 2, window_out.shape[1]
    half = half_ref[0]
    copies = start_sources(packs, small_ref, sem)
    unpack = functools.partial(read_sources, copies, small_ref, at_ref, weight_ref)
    blocks = blocks_of(state, None if gathered else half, count, rows)
    d_halves(sums, half, fc_ref, dsum_ref, dhalf_ref, count)
    factor = gradients(blocks, late_ref, dhalf_ref, field_ref, rows, cols)
    masks = []
    for i, block in enumerate(blocks):
        theta = block() - get_block(field_ref, i, rows) * factor
        if i < 2:
            window_out[i * rows : (i + 1) * rows, :] = theta
            masks.append(jax.nn.sigmoid(theta).astype(jnp.bfloat16))
        else:
            rest_out[(i - 2) * rows : (i - 1) * rows, :] = theta
    image(jnp.concatenate(masks, 0), unpack, at_ref, weight_ref, (fr_ref, fc_ref, late_ref), target_ref, partial_ref, resist_ref, scratch, rows)


def last_kernel(count, n_sums, *refs):
    half_ref, refs = refs[0], refs[1:]
    sums, state, refs = refs[:n_sums], refs[n_sums : n_sums + 2], refs[n_sums + 2 :]
    fc_ref, late_ref, resist_ref, resist_other, theta_out, resist_out, field_ref, dsum_ref, dhalf_ref = refs
    rows, cols = theta_out.shape
    width = resist_ref.shape[1]
    half = half_ref[0]
    d_halves(sums, half, fc_ref, dsum_ref, dhalf_ref, count)
    factor = gradients(blocks_of(state, None, count, rows), late_ref, dhalf_ref, field_ref, rows, cols)
    d_own = jnp.concatenate([get_block(field_ref, 0, rows)[HALO:], get_block(field_ref, 1, rows)[: rows - HALO]], 0)
    theta_out[...] = state[0][HALO : HALO + rows, :] - d_own * factor
    first = half == 0
    resist_out[:, :width] = jnp.where(first, resist_ref[...], resist_other[...])
    resist_out[:, width:] = jnp.where(first, resist_other[...], resist_ref[...])


def pairs_of(count):
    return [(o, count - o) for o in range(1, (count + 1) // 2)] + [(count // 2, count // 2)] * (count % 2 == 0)


def fetch(array, low, high, across=0):
    strips, size = lax.axis_size("strip"), lax.axis_size("src")
    steps = [
        ((z + (high if s % SPLIT else low)) % strips * size + (s + SPLIT * across) % size, z * size + s)
        for z in range(strips)
        for s in range(size)
    ]
    return lax.ppermute(array, ("strip", "src"), steps)


def exchange(partial, half, dtype):
    total = (partial + partner(partial)).astype(dtype)
    sums = [total]
    for low, high in pairs_of(lax.axis_size("strip")):
        send = total
        if low == high:
            send = jnp.where(half == 0, total[:, :FREQ], total[:, FREQ:])
        mine = fetch(send, low, high)
        sums += [mine, partner(mine)]
    return sums


def per_device_body(theta, target, source_shift, source_weight):
    rows, cols = theta.shape
    count = lax.axis_size("strip")
    n_src = lax.axis_size("src")
    width = cols // SPLIT
    sources = source_weight.shape[0] * n_src
    half = (lax.axis_index("src") % SPLIT).astype(jnp.int32)
    forward_rows, forward_cols, late = [jnp.asarray(t) for t in build_tables(rows, cols)]
    vmem = pl.BlockSpec(memory_space=pltpu.VMEM)
    smem = pl.BlockSpec(memory_space=pltpu.SMEM)
    f32 = jnp.float32

    far_space = pl.BlockSpec(memory_space=pltpu.HBM)
    low = jnp.bfloat16
    outs = [pltpu.VMEM(a.shape, a.dtype) for a in (forward_rows, forward_cols)]
    outs += [pltpu.VMEM((late.shape[0] - (SPLIT - 1) * 4 * FREQ, late.shape[1]), late.dtype)]
    outs += [pltpu.VMEM((rows, width), jnp.int32), pltpu.VMEM(theta.shape, f32)]
    outs += [pltpu.VMEM((HALO, cols), low), pltpu.VMEM((3 * HALO, cols), low), pltpu.VMEM((HALO, cols), low)]
    outs += [pltpu.VMEM((8, FREQ), f32)]
    forward_rows, forward_cols, late, target, theta, halo, near, far, pack = pl.pallas_call(
        prepare_kernel,
        out_shape=outs,
        in_specs=[smem] + [far_space] * 7,
        out_specs=[vmem] * len(outs),
        scratch_shapes=[
            pltpu.SMEM(source_shift.shape[::-1], jnp.int32),
            pltpu.SMEM(source_weight.shape, f32),
            pltpu.SemaphoreType.DMA((10,)),
        ],
        name="prepare",
    )(half.reshape(1), source_shift.T, source_weight, theta, forward_rows, forward_cols, late, target)
    mine = fetch(halo, count - 1, 1)
    packs = [pack] + [shifted(pack, "src", SPLIT * k) for k in range(1, n_src // SPLIT)]
    packs = [a for one in packs for a in (one, partner(one))]
    halo = [mine, partner(mine)]
    fetched = [fetch(near, count - 1, 1)]
    fetched += [fetch(far, o, o) for o in range(2, count - 1)]
    pieces = [a for mine in fetched for a in (mine, partner(mine))]

    source_scratch = [
        pltpu.SMEM((3, sources), jnp.int32),
        pltpu.SMEM((sources,), f32),
        pltpu.SMEM((n_src, 8, FREQ), f32),
        pltpu.SemaphoreType.DMA((n_src,)),
    ]
    image_scratch = [
        pltpu.VMEM((FREQ, 2 * FREQ), f32),
        pltpu.VMEM((sources, SPAN, FREQ), f32),
        pltpu.VMEM((sources, 2 * SPAN, width), jnp.bfloat16),
        pltpu.VMEM((sources, 2 * rows, width), f32),
        pltpu.VMEM((sources, SPAN, 2 * width), jnp.bfloat16),
        pltpu.VMEM((rows, width), f32),
        pltpu.VMEM((FREQ, 2 * FREQ), f32),
    ]
    adjoint_scratch = [
        pltpu.VMEM((2 * count * HALF, 2 * FREQ), jnp.bfloat16),
        pltpu.VMEM((count, 2 * FREQ, cols), jnp.bfloat16),
    ]

    def call(kernel, args, outs, scratch, flops):
        outs = [jax.ShapeDtypeStruct(shape, dtype) for shape, dtype in outs]
        arrays = [*args, *outs, *[a for a in scratch if a.dtype in (f32, jnp.bfloat16)]]
        held = sum(math.prod(a.shape) * jnp.dtype(a.dtype).itemsize for a in arrays)
        return pl.pallas_call(
            kernel,
            out_shape=outs,
            in_specs=[smem] + [vmem] * (len(args) - 1),
            out_specs=[vmem] * len(outs),
            scratch_shapes=scratch,
            compiler_params=pltpu.CompilerParams(vmem_limit_bytes=held + (6 << 20)),
            cost_estimate=pl.CostEstimate(flops=flops, bytes_accessed=4 << 20, transcendentals=1 << 20),
        )(*args)

    smalls = [half.reshape(1), *packs]
    n_packs = len(packs)
    partial_shape = ((FOLD, 2 * FREQ), f32)
    (partial,) = call(
        functools.partial(first_kernel, n_packs),
        [*smalls, *halo, theta, forward_rows, forward_cols, late, target],
        [partial_shape],
        source_scratch + image_scratch,
        6 << 30,
    )
    state, gathered = [theta, *pieces], False
    for _ in range(ITERS - 1):
        sums = exchange(partial, half, f32)
        partial, resist, *state = call(
            functools.partial(later_kernel, count, n_packs, len(sums), len(state), gathered),
            [*smalls, *sums, *state, forward_rows, forward_cols, late, target],
            [partial_shape, ((rows, width), f32), ((2 * rows, cols), f32), (((count - 2) * rows, cols), f32)],
            source_scratch + image_scratch + adjoint_scratch,
            6 << 30,
        )
        gathered = True
    sums = exchange(partial, half, jnp.bfloat16)
    resist_other = partner(resist)
    theta, resist = call(
        functools.partial(last_kernel, count, len(sums)),
        [half.reshape(1), *sums, *state, forward_cols, late, resist, resist_other],
        [((rows, cols), f32)] * 2,
        [pltpu.VMEM((SPLIT * count, rows, width), f32)] + adjoint_scratch,
        1 << 30,
    )
    return (theta, resist)


def solution(mesh):
    return jax.shard_map(
        per_device_body,
        mesh=mesh,
        in_specs=(P(("band", "strip"), None), P(("band", "strip"), None), P("src", None), P("src")),
        out_specs=(P(("band", "strip"), None), P(("band", "strip"), None)),
        check_vma=False,
    )
```
